128 devices in a mesh: gx: 4 (over z_lo, core), gy: 8 (over z_hi, y), gz: 4 (over x).
Axes of the slice: x: 4, y: 4, z: 4 (z_hi: 2, z_lo: 2; z = z_hi * 2 + z_lo), core: 2. Of those that a mesh axis runs over, the one named last changes fastest.
Arguments:
- cell_volume: float32 [64, 128, 512], P('gx', 'gy', 'gz'), may hold values from 0.5 to 2
- exponent: int32 [64, 128, 512], P('gx', 'gy', 'gz'), may hold values from 0 to 7
- owner_row: int32 [32768], P(('gx', 'gy', 'gz')), may hold values from 0 to 32767, as said below
Outputs:
- stencil_out: float32 [27, 32768, 128], P(None, ('gx', 'gy', 'gz'))
- lumped_out: float32 [32768, 128], P(('gx', 'gy', 'gz'))
The draws below stay inside these ranges and needn't reach their ends.
Inputs may be any that keep to these rules, and one draw needn't show every extreme that they name: owner_row is a permutation of the row blocks; the row blocks of each device's share of owner_row go to each owner (owner_row // 256) exactly 2 times.
All inputs are finite; a program needn't handle non-finite values.
Results may differ from the reference program's by a relative error of at most 0.00007.
Values sent between devices are 32-bit elements; how exact they have to be, the bound alone decides.
A program may use at most 64 MiB of HBM per device.

```python
import math
import jax
import jax.numpy as jnp

EX = 16
EY = 16
EZ = 128
NX = 64
NY = 128
NZ = 512
LINES_DEV = 256
LINES = 32768
SENDS = 2
N_GX = 4
N_GY = 8
N_GZ = 4
DEVICES = 128


def draw_owner_row(key, part):
    source_keys = jax.random.split(jax.random.fold_in(key, 101), DEVICES)
    target_keys = jax.random.split(jax.random.fold_in(key, 202), DEVICES)
    source_perm = jax.vmap(lambda subkey: jax.random.permutation(subkey, LINES_DEV))(source_keys)
    target_perm = jax.vmap(lambda subkey: jax.random.permutation(subkey, LINES_DEV))(target_keys)
    owner_dev = source_perm % DEVICES
    rank_ids = source_perm // DEVICES
    source_ids = jnp.arange(DEVICES, dtype=jnp.int32)[:, None]
    slot_ids = target_perm[owner_dev, source_ids * SENDS + rank_ids]
    return (owner_dev * LINES_DEV + slot_ids).reshape(-1).astype(jnp.int32)


def with_ends(drawn, key, least, high):
    longest = drawn.shape.index(max(drawn.shape))
    spots = []
    for shift in (0, 1):
        where = [jax.random.randint(jax.random.fold_in(key, axis), (), 0, length) for axis, length in enumerate(drawn.shape)]
        where[longest] = (where[longest] + shift) % drawn.shape[longest]
        spots.append(tuple(where))
    return drawn.at[spots[0]].set(least).at[spots[1]].set(high)


def shard_levels(own_key, shape, cuts, low, top_value):
    level, own = 1.0, jax.random.fold_in(own_key, 6)
    for dim, shards_of in cuts:
        draws = jnp.exp(jax.random.uniform(jax.random.fold_in(own, dim), (shards_of,), jnp.float32, low / len(cuts), top_value / len(cuts)))
        level = level * jnp.repeat(draws, shape[dim] // shards_of).reshape([-1 if axis == dim else 1 for axis in range(len(shape))])
    return level


def setup_inputs(seed: int = 0) -> dict:
    key_of = jax.random.split(jax.random.key(seed), 4)
    return {
        "cell_volume": jnp.clip(jnp.exp(math.log(2.0) - 1.3862944 * jax.random.uniform(key_of[0], (NX, NY, NZ), jnp.float32) ** shard_levels(key_of[0], (NX, NY, NZ), ((0, 4), (1, 8), (2, 4)), -0.2, 0.2)), 0.5, 2.0),
        "exponent": with_ends(jax.random.randint(key_of[1], (NX, NY, NZ), 0, 8), jax.random.fold_in(key_of[1], 1), 0, 7).astype(jnp.int32),
        "owner_row": draw_owner_row(jax.random.fold_in(key_of[3], 71), 0),
    }


log_step = 0.3


def reference(cell_volume, exponent, owner_row):
    weight = cell_volume * jnp.exp(-log_step * exponent.astype(jnp.float32))
    current = weight[None, None, None]
    for along in range(3):
        behind = jnp.roll(current, 1, axis=3 + along)
        current = jnp.concatenate([behind, 2.0 * (current + behind), current], axis=along)
    stencil = current.reshape(27, NX, NY, NZ) * 0.015625
    lumped = 1.0 / jnp.sum(stencil, axis=0)
    stencil_lines = stencil.reshape(27, N_GX, EX, N_GY, EY, N_GZ, EZ).transpose(0, 1, 3, 5, 2, 4, 6).reshape(27, LINES, EZ)
    lumped_lines = lumped.reshape(N_GX, EX, N_GY, EY, N_GZ, EZ).transpose(0, 2, 4, 1, 3, 5).reshape(LINES, EZ)
    stencil_out = jnp.zeros((27, LINES, EZ), jnp.float32).at[:, owner_row].set(stencil_lines)
    lumped_out = jnp.zeros((LINES, EZ), jnp.float32).at[owner_row].set(lumped_lines)
    return (stencil_out, lumped_out)
```

```python
import jax
import jax.numpy as jnp
from jax import lax
from jax.experimental import pallas as pl
from jax.experimental.pallas import tpu as pltpu
from jax.sharding import PartitionSpec as P

MESH = pl.DeviceIdType.MESH
AXES = ("gx", "gy", "gz")
LOG_STEP = 0.3
NX, NY, NZ = 4, 8, 4
DEV = NX * NY * NZ
SPAN = 16
ROWS = SPAN * SPAN
LANES = 128
PARTS = 5
CHUNKS = 4
HALO = ((1, 0, 0), (0, 1, 0), (1, 1, 0), (0, 0, 1), (1, 0, 1), (0, 1, 1), (1, 1, 1))

f32, bf16, i32 = jnp.float32, jnp.bfloat16, jnp.int32


def pieces(x):
    high = x.astype(bf16)
    rest = x - high.astype(f32)
    middle = rest.astype(bf16)
    low = (rest - middle.astype(f32)).astype(bf16)
    return high, middle, low


def dot_t(a, b):
    return lax.dot_general(a, b, (((1,), (1,)), ((), ())), preferred_element_type=f32)


def dot_n(a, b):
    return lax.dot_general(a, b, (((1,), (0,)), ((), ())), preferred_element_type=f32)


def pick(select, x):
    return sum(dot_n(select, piece) for piece in pieces(x))


def pick_t(select, x):
    return sum(dot_t(select, piece) for piece in pieces(x))


def exchange(
    volume_hbm, exponent_hbm, owner_hbm, got,
    volume, exponent, owner, weight, y_layer, edge,
    x_got, y_got, xy_got, z_got, packed,
    in_sems, halo_send, halo_recv, send_sem, recv_sem, own_sem,
):
    me = tuple(lax.axis_index(axis) for axis in AXES)
    my_dev = (me[0] * NY + me[1]) * NZ + me[2]

    def ahead(x, y, z):
        return (lax.rem(me[0] + x, NX), lax.rem(me[1] + y, NY), lax.rem(me[2] + z, NZ))

    def peer(step):
        return ahead(step // (NY * NZ), lax.rem(step // NZ, NY), lax.rem(step, NZ))

    loads = [
        pltpu.make_async_copy(src, dst, in_sems.at[n])
        for n, (src, dst) in enumerate(
            ((volume_hbm, volume), (exponent_hbm, exponent), (owner_hbm, owner))
        )
    ]
    for load in loads:
        load.start()

    barrier = pltpu.get_barrier_semaphore()

    def greet(step, carry):
        pl.semaphore_signal(barrier, inc=1, device_id=peer(step), device_id_type=MESH)
        return carry

    lax.fori_loop(1, DEV, greet, 0)

    for load in loads:
        load.wait()
    weight[...] = volume[...] * jnp.exp(-LOG_STEP * exponent[...].astype(f32))
    y_layer[...] = weight[pl.ds(SPAN - 1, SPAN, stride=SPAN), :]
    last = (lax.broadcasted_iota(i32, (8, LANES), 1) == LANES - 1).astype(bf16)
    edge[...] = pick_t(last, weight[...])[0:1]

    rows = lax.broadcasted_iota(i32, (ROWS, ROWS), 0)
    columns = lax.broadcasted_iota(i32, (ROWS, ROWS), 1)
    owner_dev = owner[...] // ROWS
    slots = (owner[...] - owner_dev * ROWS).astype(f32)
    same = owner_dev == rows // 2
    before = (rows < columns).astype(bf16)
    rank = dot_n(same.astype(bf16), before)
    order = jnp.where(same & (rank == (rows % 2).astype(f32)), 1.0, 0.0).astype(bf16)

    pl.semaphore_wait(barrier, DEV - 1)
    sources = (
        weight.at[pl.ds(ROWS - SPAN, SPAN)], y_layer, weight.at[pl.ds(ROWS - 8, 8)],
        edge, edge, edge, edge,
    )
    targets = (x_got, y_got, xy_got, z_got.at[0], z_got.at[1], z_got.at[2], z_got.at[3])
    halos = []
    for n, step in enumerate(HALO):
        copy = pltpu.make_async_remote_copy(
            src_ref=sources[n], dst_ref=targets[n],
            send_sem=halo_send.at[n], recv_sem=halo_recv.at[n],
            device_id=ahead(*step), device_id_type=MESH,
        )
        copy.start()
        halos.append(copy)

    packed[0] = pick(order, weight[...]).reshape(DEV, 2, LANES)
    for copy in halos:
        copy.wait()

    own = weight[...].reshape(SPAN, SPAN, LANES)
    x_layer, y_back = x_got[...], y_got[...]
    corner = xy_got[7:8]
    behind_x = jnp.concatenate([x_layer[None], own[:-1]], axis=0)
    behind_y = jnp.concatenate([y_back[:, None], own[:, :-1]], axis=1)
    y_edge = jnp.concatenate([corner, y_back[:-1]], axis=0)
    behind_xy = jnp.concatenate([y_edge[:, None], behind_x[:, :-1]], axis=1)
    for n, lines in enumerate((behind_x, behind_y, behind_xy)):
        packed[n + 1] = pick(order, lines.reshape(ROWS, LANES)).reshape(DEV, 2, LANES)

    at = lax.broadcasted_iota(i32, (1, ROWS), 1)
    first_x, first_y = at < SPAN, at % SPAN == 0
    z_own, z_x, z_y, z_xy = (z_got[n] for n in range(4))

    def turn(row, by):
        return pltpu.roll(row, by % ROWS, 1)

    z_rows = (
        z_own,
        jnp.where(first_x, turn(z_x, SPAN), turn(z_own, SPAN)),
        jnp.where(first_y, turn(z_y, 1 - SPAN), turn(z_own, 1)),
        jnp.where(
            first_x,
            jnp.where(first_y, turn(z_xy, 1), turn(z_x, SPAN + 1)),
            jnp.where(first_y, turn(z_y, 1), turn(z_own, SPAN + 1)),
        ),
        slots,
    )
    line = lax.broadcasted_iota(i32, (LANES, ROWS), 0)
    table = jnp.zeros((LANES, ROWS), f32)
    for n, row in enumerate(z_rows):
        table = jnp.where(line == n, jnp.broadcast_to(row, (LANES, ROWS)), table)
    packed[4] = pick_t(order, table).reshape(DEV, 2, LANES)

    def send(step):
        there = peer(step)
        dev = (there[0] * NY + there[1]) * NZ + there[2]
        return pltpu.make_async_remote_copy(
            src_ref=packed.at[:, dev], dst_ref=got.at[:, my_dev],
            send_sem=send_sem, recv_sem=recv_sem,
            device_id=there, device_id_type=MESH,
        )

    def start(n, carry):
        send(lax.rem(n * 37, DEV)).start()
        return carry

    lax.fori_loop(1, DEV, start, 0)
    keep = pltpu.make_async_copy(packed.at[:, my_dev], got.at[:, my_dev], own_sem)
    keep.start()
    keep.wait()

    all_others = pl.ds(0, DEV - 1)
    pltpu.make_async_remote_copy(
        src_ref=packed.at[:, all_others], dst_ref=got.at[:, all_others],
        send_sem=send_sem, recv_sem=recv_sem, device_id=me, device_id_type=MESH,
    ).wait()


def assemble(got, stencil_hbm, lumped_hbm, stencil, lumped, out_sems, lump_sem):
    rows = ROWS // CHUNKS
    extra = got[4].reshape(ROWS, LANES)
    fourth = (lax.broadcasted_iota(i32, (8, LANES), 1) == 4).astype(bf16)
    slot = dot_t(fourth, extra.astype(bf16))[0:1]
    line_pieces = [pieces(got[n].reshape(ROWS, LANES)) for n in range(PARTS)]
    lane = lax.broadcasted_iota(i32, (rows, LANES), 1)
    copies = []
    for chunk in range(CHUNKS):
        here = pl.ds(chunk * rows, rows)
        mine = lax.broadcasted_iota(i32, (rows, ROWS), 0) + chunk * rows
        place = jnp.where(slot == mine.astype(f32), 1.0, 0.0).astype(bf16)
        placed = [sum(dot_n(place, piece) for piece in three) for three in line_pieces]
        lines, tail = placed[:4], placed[4]
        now = [line * 0.015625 for line in lines]
        behind = [
            jnp.where(lane == 0, tail[:, n : n + 1] * 0.015625, pltpu.roll(line, 1, 1))
            for n, line in enumerate(now)
        ]
        total = sum(now) + sum(behind)
        lumped[here, :] = 1.0 / (27.0 * total)

        def spread(current, back):
            return (back, 2.0 * (current + back), current)

        def plane(four):
            along = zip(spread(four[0], four[1]), spread(four[2], four[3]))
            return [value for current, back in along for value in spread(current, back)]

        for n, (current, back) in enumerate(zip(plane(now), plane(behind))):
            for k, value in enumerate(spread(current, back)):
                stencil[3 * n + k, here, :] = value
        copy = pltpu.make_async_copy(
            stencil.at[:, here], stencil_hbm.at[:, here], out_sems.at[chunk]
        )
        copy.start()
        copies.append(copy)
    copy = pltpu.make_async_copy(lumped, lumped_hbm, lump_sem)
    copy.start()
    copies.append(copy)
    for copy in copies:
        copy.wait()


def shards(cell_volume, exponent, owner_row):
    vmem = pl.BlockSpec(memory_space=pltpu.VMEM)
    hbm = pl.BlockSpec(memory_space=pltpu.HBM)
    dma = pltpu.SemaphoreType.DMA
    got = pl.pallas_call(
        exchange,
        name="exchange",
        out_shape=jax.ShapeDtypeStruct((PARTS, DEV, 2, LANES), f32),
        in_specs=[hbm] * 3,
        out_specs=vmem,
        scratch_shapes=[
            pltpu.VMEM((ROWS, LANES), f32),
            pltpu.VMEM((ROWS, LANES), i32),
            pltpu.VMEM((1, ROWS), i32),
            pltpu.VMEM((ROWS, LANES), f32),
            pltpu.VMEM((SPAN, LANES), f32),
            pltpu.VMEM((1, ROWS), f32),
            pltpu.VMEM((SPAN, LANES), f32),
            pltpu.VMEM((SPAN, LANES), f32),
            pltpu.VMEM((8, LANES), f32),
            pltpu.VMEM((4, 1, ROWS), f32),
            pltpu.VMEM((PARTS, DEV, 2, LANES), f32),
            dma((3,)), dma((7,)), dma((7,)), dma, dma, dma,
        ],
        compiler_params=pltpu.CompilerParams(has_side_effects=True, collective_id=1),
    )(
        cell_volume.reshape(ROWS, LANES),
        exponent.reshape(ROWS, LANES),
        owner_row.reshape(1, ROWS),
    )
    return pl.pallas_call(
        assemble,
        name="assemble",
        out_shape=(
            jax.ShapeDtypeStruct((27, ROWS, LANES), f32),
            jax.ShapeDtypeStruct((ROWS, LANES), f32),
        ),
        in_specs=[vmem],
        out_specs=(hbm, hbm),
        scratch_shapes=[
            pltpu.VMEM((27, ROWS, LANES), f32),
            pltpu.VMEM((ROWS, LANES), f32),
            dma((CHUNKS,)), dma,
        ],
    )(got)


def solution(mesh):
    return jax.shard_map(
        shards,
        mesh=mesh,
        in_specs=(P(*AXES), P(*AXES), P(AXES)),
        out_specs=(P(None, AXES, None), P(AXES, None)),
        check_vma=False,
    )
```

```python
import jax
import jax.numpy as jnp
from jax import lax
from jax.experimental import pallas as pl
from jax.experimental.pallas import tpu as pltpu
from jax.sharding import PartitionSpec as P

LOGICAL = pl.DeviceIdType.LOGICAL
AXES = ("gx", "gy", "gz")
LOG_STEP = 0.3
NX, NY, NZ = 4, 8, 4
DEV = NX * NY * NZ
SPAN = 16
ROWS = SPAN * SPAN
LANES = 128
PARTS = 5
CHUNKS = 4
ROOT = (3 * NY + 6) * NZ + 2
HALO = ((1, 0, 0), (0, 1, 0), (1, 1, 0), (0, 0, 1), (1, 0, 1), (0, 1, 1), (1, 1, 1))

f32, bf16, i32 = jnp.float32, jnp.bfloat16, jnp.int32


def pieces(x):
    high = x.astype(bf16)
    rest = x - high.astype(f32)
    middle = rest.astype(bf16)
    low = (rest - middle.astype(f32)).astype(bf16)
    return high, middle, low


def dot_t(a, b):
    return lax.dot_general(a, b, (((1,), (1,)), ((), ())), preferred_element_type=f32)


def dot_n(a, b):
    return lax.dot_general(a, b, (((1,), (0,)), ((), ())), preferred_element_type=f32)


def pick(select, x):
    return sum(dot_n(select, piece) for piece in pieces(x))


def pick_t(select, x):
    return sum(dot_t(select, piece) for piece in pieces(x))


def exchange(
    volume_hbm, exponent_hbm, owner_hbm, got,
    volume, exponent, owner, weight, y_layer, edge,
    x_got, y_got, xy_got, z_got, packed,
    in_sems, halo_send, halo_recv, send_sem, recv_sem, own_sem, go_sem,
):
    me = tuple(lax.axis_index(axis) for axis in AXES)
    along_x = [lax.rem(me[0] + k, NX) * (NY * NZ) for k in range(NX)]
    along_y = [lax.rem(me[1] + k, NY) * NZ for k in range(NY)]
    along_z = [lax.rem(me[2] + k, NZ) for k in range(NZ)]
    my_dev = along_x[0] + along_y[0] + along_z[0]
    is_root = my_dev == ROOT

    def ahead(x, y, z):
        return along_x[x % NX] + along_y[y % NY] + along_z[z % NZ]

    others = [
        ahead(step // (NY * NZ), step // NZ, step)
        for step in ((n * 37) % DEV for n in range(1, DEV))
    ]

    loads = [
        pltpu.make_async_copy(src, dst, in_sems.at[n])
        for n, (src, dst) in enumerate(
            ((volume_hbm, volume), (exponent_hbm, exponent), (owner_hbm, owner))
        )
    ]
    for load in loads:
        load.start()

    barrier = pltpu.get_barrier_semaphore()

    greeted = jnp.int32(0)
    for x, y, z in HALO:
        source = ahead(-x, -y, -z)
        pl.semaphore_signal(barrier, inc=1, device_id=source, device_id_type=LOGICAL)
        greeted = greeted + (source == ROOT).astype(i32)

    @pl.when(jnp.logical_not(is_root) & (greeted == 0))
    def _():
        pl.semaphore_signal(barrier, inc=1, device_id=jnp.int32(ROOT), device_id_type=LOGICAL)

    for load in loads:
        load.wait()
    weight[...] = volume[...] * jnp.exp(-LOG_STEP * exponent[...].astype(f32))
    y_layer[...] = weight[pl.ds(SPAN - 1, SPAN, stride=SPAN), :]
    last = (lax.broadcasted_iota(i32, (8, LANES), 1) == LANES - 1).astype(bf16)
    edge[...] = pick_t(last, weight[...])[0:1]

    rows = lax.broadcasted_iota(i32, (ROWS, ROWS), 0)
    columns = lax.broadcasted_iota(i32, (ROWS, ROWS), 1)
    owner_dev = owner[...] // ROWS
    slots = (owner[...] - owner_dev * ROWS).astype(f32)
    same = owner_dev == rows // 2
    before = (rows < columns).astype(bf16)
    rank = dot_n(same.astype(bf16), before)
    order = jnp.where(same & (rank == (rows % 2).astype(f32)), 1.0, 0.0).astype(bf16)

    @pl.when(is_root)
    def _():
        pl.semaphore_wait(barrier, DEV - 1)

    @pl.when(jnp.logical_not(is_root))
    def _():
        pl.semaphore_wait(barrier, len(HALO))

    sources = (
        weight.at[pl.ds(ROWS - SPAN, SPAN)], y_layer, weight.at[pl.ds(ROWS - 8, 8)],
        edge, edge, edge, edge,
    )
    targets = (x_got, y_got, xy_got, z_got.at[0], z_got.at[1], z_got.at[2], z_got.at[3])
    halos = []
    for n, step in enumerate(HALO):
        copy = pltpu.make_async_remote_copy(
            src_ref=sources[n], dst_ref=targets[n],
            send_sem=halo_send.at[n], recv_sem=halo_recv.at[n],
            device_id=ahead(*step), device_id_type=LOGICAL,
        )
        copy.start()
        halos.append(copy)

    @pl.when(is_root)
    def _():
        for there in others:
            pl.semaphore_signal(go_sem, inc=1, device_id=there, device_id_type=LOGICAL)

    packed[0] = pick(order, weight[...]).reshape(DEV, 2, LANES)
    for copy in halos:
        copy.wait()

    own = weight[...].reshape(SPAN, SPAN, LANES)
    x_layer, y_back = x_got[...], y_got[...]
    corner = xy_got[7:8]
    behind_x = jnp.concatenate([x_layer[None], own[:-1]], axis=0)
    behind_y = jnp.concatenate([y_back[:, None], own[:, :-1]], axis=1)
    y_edge = jnp.concatenate([corner, y_back[:-1]], axis=0)
    behind_xy = jnp.concatenate([y_edge[:, None], behind_x[:, :-1]], axis=1)
    for n, lines in enumerate((behind_x, behind_y, behind_xy)):
        packed[n + 1] = pick(order, lines.reshape(ROWS, LANES)).reshape(DEV, 2, LANES)

    at = lax.broadcasted_iota(i32, (1, ROWS), 1)
    first_x, first_y = at < SPAN, at % SPAN == 0
    z_own, z_x, z_y, z_xy = (z_got[n] for n in range(4))

    def turn(row, by):
        return pltpu.roll(row, by % ROWS, 1)

    z_rows = (
        z_own,
        jnp.where(first_x, turn(z_x, SPAN), turn(z_own, SPAN)),
        jnp.where(first_y, turn(z_y, 1 - SPAN), turn(z_own, 1)),
        jnp.where(
            first_x,
            jnp.where(first_y, turn(z_xy, 1), turn(z_x, SPAN + 1)),
            jnp.where(first_y, turn(z_y, 1), turn(z_own, SPAN + 1)),
        ),
        slots,
    )
    line = lax.broadcasted_iota(i32, (LANES, ROWS), 0)
    table = jnp.zeros((LANES, ROWS), f32)
    for n, row in enumerate(z_rows):
        table = jnp.where(line == n, jnp.broadcast_to(row, (LANES, ROWS)), table)
    packed[4] = pick_t(order, table).reshape(DEV, 2, LANES)

    @pl.when(jnp.logical_not(is_root))
    def _():
        pl.semaphore_wait(go_sem, 1)

    for there in others:
        pltpu.make_async_remote_copy(
            src_ref=packed.at[:, there], dst_ref=got.at[:, my_dev],
            send_sem=send_sem, recv_sem=recv_sem,
            device_id=there, device_id_type=LOGICAL,
        ).start()
    keep = pltpu.make_async_copy(packed.at[:, my_dev], got.at[:, my_dev], own_sem)
    keep.start()
    keep.wait()

    all_others = pl.ds(0, DEV - 1)
    pltpu.make_async_remote_copy(
        src_ref=packed.at[:, all_others], dst_ref=got.at[:, all_others],
        send_sem=send_sem, recv_sem=recv_sem, device_id=my_dev, device_id_type=LOGICAL,
    ).wait()


def assemble(got, stencil_hbm, lumped_hbm, stencil, lumped, out_sems, lump_sem):
    rows = ROWS // CHUNKS
    extra = got[4].reshape(ROWS, LANES)
    fourth = (lax.broadcasted_iota(i32, (8, LANES), 1) == 4).astype(bf16)
    slot = dot_t(fourth, extra.astype(bf16))[0:1]
    line_pieces = [pieces(got[n].reshape(ROWS, LANES)) for n in range(PARTS)]
    lane = lax.broadcasted_iota(i32, (rows, LANES), 1)
    copies = []
    for chunk in range(CHUNKS):
        here = pl.ds(chunk * rows, rows)
        mine = lax.broadcasted_iota(i32, (rows, ROWS), 0) + chunk * rows
        place = jnp.where(slot == mine.astype(f32), 1.0, 0.0).astype(bf16)
        placed = [sum(dot_n(place, piece) for piece in three) for three in line_pieces]
        lines, tail = placed[:4], placed[4]
        now = [line * 0.015625 for line in lines]
        behind = [
            jnp.where(lane == 0, tail[:, n : n + 1] * 0.015625, pltpu.roll(line, 1, 1))
            for n, line in enumerate(now)
        ]
        total = sum(now) + sum(behind)
        lumped[here, :] = 1.0 / (27.0 * total)

        def spread(current, back):
            return (back, 2.0 * (current + back), current)

        def plane(four):
            along = zip(spread(four[0], four[1]), spread(four[2], four[3]))
            return [value for current, back in along for value in spread(current, back)]

        for n, (current, back) in enumerate(zip(plane(now), plane(behind))):
            for k, value in enumerate(spread(current, back)):
                stencil[3 * n + k, here, :] = value
        copy = pltpu.make_async_copy(
            stencil.at[:, here], stencil_hbm.at[:, here], out_sems.at[chunk]
        )
        copy.start()
        copies.append(copy)
    copy = pltpu.make_async_copy(lumped, lumped_hbm, lump_sem)
    copy.start()
    copies.append(copy)
    for copy in copies:
        copy.wait()


def in_hbm(x):
    return pltpu.with_memory_space_constraint(x, pltpu.HBM)


def shards(cell_volume, exponent, owner_row):
    vmem = pl.BlockSpec(memory_space=pltpu.VMEM)
    hbm = pl.BlockSpec(memory_space=pltpu.HBM)
    dma = pltpu.SemaphoreType.DMA
    got = pl.pallas_call(
        exchange,
        name="exchange",
        out_shape=pltpu.VMEM((PARTS, DEV, 2, LANES), f32),
        in_specs=[hbm] * 3,
        out_specs=vmem,
        scratch_shapes=[
            pltpu.VMEM((ROWS, LANES), f32),
            pltpu.VMEM((ROWS, LANES), i32),
            pltpu.VMEM((1, ROWS), i32),
            pltpu.VMEM((ROWS, LANES), f32),
            pltpu.VMEM((SPAN, LANES), f32),
            pltpu.VMEM((1, ROWS), f32),
            pltpu.VMEM((SPAN, LANES), f32),
            pltpu.VMEM((SPAN, LANES), f32),
            pltpu.VMEM((8, LANES), f32),
            pltpu.VMEM((4, 1, ROWS), f32),
            pltpu.VMEM((PARTS, DEV, 2, LANES), f32),
            dma((3,)), dma((7,)), dma((7,)), dma, dma, dma, pltpu.SemaphoreType.REGULAR,
        ],
        compiler_params=pltpu.CompilerParams(has_side_effects=True, collective_id=1, vmem_limit_bytes=16 << 20),
    )(
        in_hbm(cell_volume.reshape(ROWS, LANES)),
        in_hbm(exponent.reshape(ROWS, LANES)),
        in_hbm(owner_row.reshape(1, ROWS)),
    )
    return pl.pallas_call(
        assemble,
        name="assemble",
        out_shape=(
            jax.ShapeDtypeStruct((27, ROWS, LANES), f32),
            jax.ShapeDtypeStruct((ROWS, LANES), f32),
        ),
        in_specs=[vmem],
        out_specs=(hbm, hbm),
        scratch_shapes=[
            pltpu.VMEM((27, ROWS, LANES), f32),
            pltpu.VMEM((ROWS, LANES), f32),
            dma((CHUNKS,)), dma,
        ],
        compiler_params=pltpu.CompilerParams(vmem_limit_bytes=16 << 20),
    )(got)


def solution(mesh):
    return jax.shard_map(
        shards,
        mesh=mesh,
        in_specs=(P(*AXES), P(*AXES), P(AXES)),
        out_specs=(P(None, AXES, None), P(AXES, None)),
        check_vma=False,
    )
```

```python
import jax
import jax.numpy as jnp
from jax import lax
from jax.experimental import pallas as pl
from jax.experimental.pallas import tpu as pltpu
from jax.sharding import PartitionSpec as P

LOGICAL = pl.DeviceIdType.LOGICAL
AXES = ("gx", "gy", "gz")
LOG_STEP = 0.3
NX, NY, NZ = 4, 8, 4
DEV = NX * NY * NZ
HALF = NY // 2
PLANES = 4
ROOT = (3 * NY + 6) * NZ + 2
EARLY_ROOT = (3 * NY + 2) * NZ + 2
MID_ROOT = (0 * NY + 6) * NZ + 2
FIRST = (NY * NZ, 0)
SPAN = 16
ROWS = SPAN * SPAN
LANES = 128
PARTS = 9
CHUNKS = 4
HALO = ((1, 0, 0), (0, 1, 0), (1, 1, 0), (0, 0, 1), (1, 0, 1), (0, 1, 1), (1, 1, 1))

f32, bf16, i32 = jnp.float32, jnp.bfloat16, jnp.int32


def pieces(x):
    high = x.astype(bf16)
    return high, (x - high.astype(f32)).astype(bf16)


def dot_t(a, b):
    return lax.dot_general(a, b, (((1,), (1,)), ((), ())), preferred_element_type=f32)


def dot_n(a, b):
    return lax.dot_general(a, b, (((1,), (0,)), ((), ())), preferred_element_type=f32)


def pick(select, x):
    both = dot_n(select, jnp.concatenate(pieces(x), axis=1))
    return both[:, :LANES] + both[:, LANES:]


def pick_t(select, x):
    return sum(dot_t(select, piece) for piece in pieces(x))


def iota(shape, axis):
    return lax.broadcasted_iota(i32, shape, axis)


def one_hot(mask, value=1.0):
    return jnp.where(mask, value, 0.0).astype(bf16)


def exchange(
    volume_hbm, exponent_hbm, owner_hbm, got,
    volume, exponent, owner, weight, y_layer, edge,
    lines_got, z_got, packed,
    in_sems, halo_send, halo_recv, send_sem, recv_sem, own_sem, go_sem, mid_sem, early_sem,
):
    loads = [
        pltpu.make_async_copy(src, dst, in_sems.at[n])
        for n, (src, dst) in enumerate(
            ((volume_hbm, volume), (exponent_hbm, exponent), (owner_hbm, owner))
        )
    ]
    for load in loads:
        load.start()

    me = tuple(lax.axis_index(axis) for axis in AXES)
    my_dev = (me[0] * NY + me[1]) * NZ + me[2]
    is_root, is_mid_root, is_early_root = (
        my_dev == root for root in (ROOT, MID_ROOT, EARLY_ROOT)
    )
    my_plane = me[0] // 2 + 2 * (me[1] // HALF)
    is_early, is_mid, is_late = my_plane < 2, my_plane == 2, my_plane == 3
    not_ = jnp.logical_not

    def ahead(x, y, z):
        there_x = lax.rem(me[0] + x % NX, NX)
        there_y = lax.rem(me[1] + y % NY, NY)
        there_z = lax.rem(me[2] + z % NZ, NZ)
        return (there_x * NY + there_y) * NZ + there_z

    def signal(sem, there):
        pl.semaphore_signal(sem, inc=1, device_id=there, device_id_type=LOGICAL)

    barrier = pltpu.get_barrier_semaphore()
    sources = [ahead(-x, -y, -z) for x, y, z in HALO]
    def greet(root, wanted):
        known = sum((source == root).astype(i32) for source in sources)

        @pl.when(wanted & (my_dev != root) & (known == 0))
        def _():
            signal(barrier, jnp.int32(root))

    greet(ROOT, my_dev >= 0)
    greet(MID_ROOT, not_(is_late))
    greet(EARLY_ROOT, is_early)
    for source in sources:
        signal(barrier, source)

    def plane(number):
        z_hi, z_lo = number // 2, number % 2
        core, y = lax.rem(me[0], 2), lax.rem(me[1], HALF)
        base_x = [(z_lo * 2 + lax.rem(core + k, 2)) * (NY * NZ) for k in range(2)]
        base_y = [(z_hi * HALF + lax.rem(y + k, HALF)) * NZ for k in range(HALF)]
        base_z = [lax.rem(me[2] + k, NZ) for k in range(NZ)]
        members = 2 * HALF * NZ
        here = my_plane == number
        for n in range(members):
            step = n * 13 % members
            there = base_x[step % 2] + base_y[step // 2 % HALF] + base_z[step // (2 * HALF)]
            yield (here if step == 0 else None), there

    def visit(planes, act, first=()):
        for there in first:
            pl.when(my_dev != there)(lambda: act(jnp.int32(there)))
        for number in planes:
            for self_at, there in plane(number):
                go = None if self_at is None else not_(self_at)
                if number == 0:
                    for known in first:
                        go = there != known if go is None else go & (there != known)
                if go is None:
                    act(there)
                else:
                    pl.when(go)(lambda: act(there))

    for load in loads:
        load.wait()
    weight[...] = volume[...] * jnp.exp(-LOG_STEP * exponent[...].astype(f32))
    y_layer[...] = weight[pl.ds(SPAN - 1, SPAN, stride=SPAN), :]
    last = one_hot(iota((8, LANES), 1) == LANES - 1)
    edge[...] = pick_t(last, weight[...])[0:1]

    @pl.when(is_root)
    def _():
        pl.semaphore_wait(barrier, DEV - 1)

    @pl.when(is_mid_root)
    def _():
        pl.semaphore_wait(barrier, DEV // 4 * 3 - 1)

    @pl.when(is_early_root)
    def _():
        pl.semaphore_wait(barrier, DEV // 2 - 1)

    @pl.when(not_(is_root | is_mid_root | is_early_root))
    def _():
        pl.semaphore_wait(barrier, len(HALO))

    halo_from = (
        weight.at[pl.ds(ROWS - SPAN, SPAN)], y_layer, weight.at[pl.ds(ROWS - 8, 8)],
        edge, edge, edge, edge,
    )
    halo_to = (
        lines_got.at[pl.ds(0, SPAN)], lines_got.at[pl.ds(SPAN, SPAN)],
        lines_got.at[pl.ds(2 * SPAN, 8)], *(z_got.at[n] for n in range(4)),
    )
    halos = []
    for n, step in enumerate(HALO):
        copy = pltpu.make_async_remote_copy(
            src_ref=halo_from[n], dst_ref=halo_to[n],
            send_sem=halo_send.at[n], recv_sem=halo_recv.at[n],
            device_id=ahead(*step), device_id_type=LOGICAL,
        )
        copy.start()
        halos.append(copy)

    @pl.when(is_early_root)
    def _():
        visit((0, 1), lambda there: signal(early_sem, there))

    @pl.when(is_mid_root)
    def _():
        visit((0, 1, 2), lambda there: signal(mid_sem, there), FIRST)

    @pl.when(is_root)
    def _():
        visit((0, 1, 3, 2), lambda there: signal(go_sem, there), FIRST)

    owner_dev = owner[...] // ROWS
    slots = (owner[...] - owner_dev * ROWS).astype(f32)
    same = owner_dev == iota((DEV, ROWS), 0)
    before = one_hot(iota((ROWS, ROWS), 0) < iota((ROWS, ROWS), 1))
    rank = dot_n(one_hot(same), before)
    ranked = [one_hot(same & (rank == value)) for value in (0.0, 1.0)]
    order = jnp.concatenate(ranked, axis=0)

    def put(part, rows):
        packed[2 * part] = rows[:DEV]
        packed[2 * part + 1] = rows[DEV:]

    own = weight[...].reshape(SPAN, SPAN, LANES)
    put(0, pick(order, weight[...]))

    def send(first, count):
        def act(there):
            pltpu.make_async_remote_copy(
                src_ref=packed.at[pl.ds(first, count), pl.ds(there, 1), :],
                dst_ref=got.at[pl.ds(first, count), pl.ds(my_dev, 1), :],
                send_sem=send_sem, recv_sem=recv_sem,
                device_id=there, device_id_type=LOGICAL,
            ).start()

        return act

    @pl.when(is_early & not_(is_early_root))
    def _():
        pl.semaphore_wait(early_sem, 1)

    @pl.when(is_mid & not_(is_mid_root))
    def _():
        pl.semaphore_wait(mid_sem, 1)

    @pl.when(is_late & not_(is_root))
    def _():
        pl.semaphore_wait(go_sem, 1)

    visit((0, 1), send(0, 2))

    empty = jnp.zeros((1, SPAN, LANES), f32)
    behind_x = jnp.concatenate([empty, own[:-1]], axis=0)
    column = jnp.zeros((SPAN, 1, LANES), f32)
    behind_y = jnp.concatenate([column, own[:, :-1]], axis=1)
    behind_xy = jnp.concatenate([column, behind_x[:, :-1]], axis=1)
    from_row, line = iota((ROWS, LANES), 0), iota((ROWS, LANES), 1)
    in_x, in_y = line < SPAN, (line >= SPAN) & (line < 2 * SPAN)
    wanted = (
        jnp.where(in_x, line, -1),
        jnp.where(in_y, (line - SPAN) * SPAN, -1),
        jnp.where(
            in_x & (line < SPAN - 1),
            line + 1,
            jnp.where(
                in_y & (line < 2 * SPAN - 1),
                (line - SPAN + 1) * SPAN,
                jnp.where(line == 2 * SPAN + 7, 0, -1),
            ),
        ),
    )
    selects = []
    for n, inner in enumerate((behind_x, behind_y, behind_xy)):
        put(n + 1, pick(order, inner.reshape(ROWS, LANES)))
        selects.append(dot_n(order, one_hot(from_row == wanted[n])).astype(bf16))
    select = jnp.concatenate(selects, axis=0)

    for copy in halos:
        copy.wait()

    pad = jnp.zeros((LANES - 2 * SPAN - 8, LANES), f32)
    rim = pick(select, jnp.concatenate([lines_got[...], pad], axis=0))
    for n in range(6):
        packed[n + 2] += rim[n * DEV : (n + 1) * DEV]

    at = iota((1, ROWS), 1)
    first_x, first_y = at < SPAN, at % SPAN == 0
    z_own, z_x, z_y, z_xy = (z_got[n] for n in range(4))

    def turn(row, by):
        return pltpu.roll(row, by % ROWS, 1)

    z_rows = (
        z_own,
        jnp.where(first_x, turn(z_x, SPAN), turn(z_own, SPAN)),
        jnp.where(first_y, turn(z_y, 1 - SPAN), turn(z_own, 1)),
        jnp.where(
            first_x,
            jnp.where(first_y, turn(z_xy, 1), turn(z_x, SPAN + 1)),
            jnp.where(first_y, turn(z_y, 1), turn(z_own, SPAN + 1)),
        ),
        slots,
    )
    table = jnp.zeros((8, ROWS), f32)
    for n, row in enumerate(z_rows):
        table = jnp.where(iota((8, ROWS), 0) == n, row, table)
    blank = jnp.zeros((LANES - 16, ROWS), f32)
    none = jnp.zeros((8, ROWS), f32)
    packed[8] = pick_t(ranked[0], jnp.concatenate([table, none, blank], axis=0)) + pick_t(
        ranked[1], jnp.concatenate([none, table, blank], axis=0)
    )

    keep = pltpu.make_async_copy(
        packed.at[:, pl.ds(my_dev, 1), :], got.at[:, pl.ds(my_dev, 1), :], own_sem
    )
    keep.start()
    visit((0, 1), send(2, PARTS - 2))

    @pl.when(is_early)
    def _():
        pl.semaphore_wait(mid_sem, 1)

    visit((2,), send(0, PARTS))

    @pl.when(not_(is_late))
    def _():
        pl.semaphore_wait(go_sem, 1)

    visit((3,), send(0, PARTS))
    keep.wait()
    all_others = pl.ds(0, DEV - 1)
    pltpu.make_async_remote_copy(
        src_ref=packed.at[:, all_others], dst_ref=got.at[:, all_others],
        send_sem=send_sem, recv_sem=recv_sem, device_id=my_dev, device_id_type=LOGICAL,
    ).wait()


def assemble(got, stencil_hbm, lumped_hbm, stencil, lumped, out_sems, lump_sem):
    rows = ROWS // CHUNKS
    extra = got[8]
    tails = [extra, pltpu.roll(extra, LANES - 8, 1)]
    slot = jnp.concatenate(
        [
            dot_t(one_hot(iota((8, LANES), 1) == 4), tail.astype(bf16))[0:1]
            for tail in tails
        ],
        axis=1,
    )
    five = [(got[2 * n], got[2 * n + 1]) for n in range(4)] + [tails]
    five = [jnp.concatenate(pieces(jnp.concatenate(two, axis=0)), axis=1) for two in five]
    lane = iota((rows, LANES), 1)
    copies = []
    for chunk in range(CHUNKS):
        here = pl.ds(chunk * rows, rows)
        mine = iota((rows, ROWS), 0) + chunk * rows
        place = one_hot(slot == mine.astype(f32), 0.015625)
        both = [dot_n(place, two) for two in five]
        placed = [pair[:, :LANES] + pair[:, LANES:] for pair in both]
        now, tail = placed[:4], placed[4]
        behind = [
            jnp.where(lane == 0, tail[:, n : n + 1], pltpu.roll(line, 1, 1))
            for n, line in enumerate(now)
        ]
        total = sum(now) + sum(behind)
        lumped[here, :] = 1.0 / (27.0 * total)

        def spread(current, back):
            return (back, 2.0 * (current + back), current)

        def plane(four):
            along = zip(spread(four[0], four[1]), spread(four[2], four[3]))
            return [value for current, back in along for value in spread(current, back)]

        for n, (current, back) in enumerate(zip(plane(now), plane(behind))):
            for k, value in enumerate(spread(current, back)):
                stencil[3 * n + k, here, :] = value
        copy = pltpu.make_async_copy(
            stencil.at[:, here], stencil_hbm.at[:, here], out_sems.at[chunk]
        )
        copy.start()
        copies.append(copy)
    copy = pltpu.make_async_copy(lumped, lumped_hbm, lump_sem)
    copy.start()
    copies.append(copy)
    for copy in copies:
        copy.wait()


def in_hbm(x):
    return pltpu.with_memory_space_constraint(x, pltpu.HBM)


def shards(cell_volume, exponent, owner_row):
    vmem = pl.BlockSpec(memory_space=pltpu.VMEM)
    hbm = pl.BlockSpec(memory_space=pltpu.HBM)
    dma, regular = pltpu.SemaphoreType.DMA, pltpu.SemaphoreType.REGULAR
    got = pl.pallas_call(
        exchange,
        name="exchange",
        out_shape=pltpu.VMEM((PARTS, DEV, LANES), f32),
        in_specs=[hbm] * 3,
        out_specs=vmem,
        scratch_shapes=[
            pltpu.VMEM((ROWS, LANES), f32),
            pltpu.VMEM((ROWS, LANES), i32),
            pltpu.VMEM((1, ROWS), i32),
            pltpu.VMEM((ROWS, LANES), f32),
            pltpu.VMEM((SPAN, LANES), f32),
            pltpu.VMEM((1, ROWS), f32),
            pltpu.VMEM((2 * SPAN + 8, LANES), f32),
            pltpu.VMEM((4, 1, ROWS), f32),
            pltpu.VMEM((PARTS, DEV, LANES), f32),
            dma((3,)), dma((7,)), dma((7,)), dma, dma, dma, regular, regular, regular,
        ],
        compiler_params=pltpu.CompilerParams(
            has_side_effects=True, collective_id=1, vmem_limit_bytes=16 << 20
        ),
    )(
        in_hbm(cell_volume.reshape(ROWS, LANES)),
        in_hbm(exponent.reshape(ROWS, LANES)),
        in_hbm(owner_row.reshape(1, ROWS)),
    )
    return pl.pallas_call(
        assemble,
        name="assemble",
        out_shape=(
            jax.ShapeDtypeStruct((27, ROWS, LANES), f32),
            jax.ShapeDtypeStruct((ROWS, LANES), f32),
        ),
        in_specs=[vmem],
        out_specs=(hbm, hbm),
        scratch_shapes=[
            pltpu.VMEM((27, ROWS, LANES), f32),
            pltpu.VMEM((ROWS, LANES), f32),
            dma((CHUNKS,)), dma,
        ],
        compiler_params=pltpu.CompilerParams(vmem_limit_bytes=16 << 20),
    )(got)


def solution(mesh):
    return jax.shard_map(
        shards,
        mesh=mesh,
        in_specs=(P(*AXES), P(*AXES), P(AXES)),
        out_specs=(P(None, AXES, None), P(AXES, None)),
        check_vma=False,
    )
```

```python
import jax
import jax.numpy as jnp
from jax import lax
from jax.experimental import pallas as pl
from jax.experimental.pallas import tpu as pltpu
from jax.sharding import PartitionSpec as P

LOGICAL = pl.DeviceIdType.LOGICAL
AXES = ("gx", "gy", "gz")
LOG_STEP = 0.3
NX, NY, NZ = 4, 8, 4
DEV = NX * NY * NZ
HALF = NY // 2
PLANES = 4
ROOT = (3 * NY + 6) * NZ + 2
EARLY_ROOT = (3 * NY + 2) * NZ + 2
MID_ROOT = (0 * NY + 6) * NZ + 2
FIRST = (NY * NZ, 0)
SPAN = 16
ROWS = SPAN * SPAN
LANES = 128
PARTS = 9
STRIDE = 13
CHUNKS = 4
HALO = ((1, 0, 0), (0, 1, 0), (1, 1, 0), (0, 0, 1), (1, 0, 1), (0, 1, 1), (1, 1, 1))

f32, bf16, i32 = jnp.float32, jnp.bfloat16, jnp.int32


def pieces(x):
    high = x.astype(bf16)
    return high, (x - high.astype(f32)).astype(bf16)


def dot_t(a, b):
    return lax.dot_general(a, b, (((1,), (1,)), ((), ())), preferred_element_type=f32)


def dot_n(a, b):
    return lax.dot_general(a, b, (((1,), (0,)), ((), ())), preferred_element_type=f32)


def pick(select, x):
    both = dot_n(select, jnp.concatenate(pieces(x), axis=1))
    return both[:, :LANES] + both[:, LANES:]


def pick_t(select, x):
    return sum(dot_t(select, piece) for piece in pieces(x))


def iota(shape, axis):
    return lax.broadcasted_iota(i32, shape, axis)


def one_hot(mask, value=1.0):
    return jnp.where(mask, value, 0.0).astype(bf16)


def exchange(
    volume_hbm, exponent_hbm, owner_hbm, got,
    volume, exponent, owner, weight, y_layer, edge,
    lines_got, z_got, packed,
    in_sems, halo_send, halo_recv, send_sem, recv_sem, own_sem, go_sem, mid_sem, early_sem,
):
    loads = [
        pltpu.make_async_copy(src, dst, in_sems.at[n])
        for n, (src, dst) in enumerate(
            ((volume_hbm, volume), (exponent_hbm, exponent), (owner_hbm, owner))
        )
    ]
    for load in loads:
        load.start()

    me = tuple(lax.axis_index(axis) for axis in AXES)
    my_dev = (me[0] * NY + me[1]) * NZ + me[2]
    is_root, is_mid_root, is_early_root = (
        my_dev == root for root in (ROOT, MID_ROOT, EARLY_ROOT)
    )
    my_plane = me[0] // 2 + 2 * (me[1] // HALF)
    is_early, is_mid, is_late = my_plane < 2, my_plane == 2, my_plane == 3
    not_ = jnp.logical_not

    def ahead(x, y, z):
        there_x = lax.rem(me[0] + x % NX, NX)
        there_y = lax.rem(me[1] + y % NY, NY)
        there_z = lax.rem(me[2] + z % NZ, NZ)
        return (there_x * NY + there_y) * NZ + there_z

    def signal(sem, there):
        pl.semaphore_signal(sem, inc=1, device_id=there, device_id_type=LOGICAL)

    barrier = pltpu.get_barrier_semaphore()
    sources = [ahead(-x, -y, -z) for x, y, z in HALO]
    def greet(root, wanted):
        known = sum((source == root).astype(i32) for source in sources)

        @pl.when(wanted & (my_dev != root) & (known == 0))
        def _():
            signal(barrier, jnp.int32(root))

    greet(ROOT, my_dev >= 0)
    greet(MID_ROOT, not_(is_late))
    greet(EARLY_ROOT, is_early)
    for source in sources:
        signal(barrier, source)

    def members(planes, side=None):
        z_hi, z_lo = planes[0] // 2, planes[0] % 2
        core, y = lax.rem(me[0], 2), lax.rem(me[1], HALF)
        if len(planes) == 2:
            base_x = [lax.rem(me[0] + k, NX) * (NY * NZ) for k in range(NX)]
            at_home = me[1] // HALF == z_hi
        else:
            base_x = [(z_lo * 2 + lax.rem(core + k, 2)) * (NY * NZ) for k in range(2)]
            at_home = my_plane == planes[0]
        if side is None:
            base_y = [(z_hi * HALF + lax.rem(y + k, HALF)) * NZ for k in range(HALF)]
        else:
            base_y = [(z_hi * HALF + side * 2 + lax.rem(y + k, 2)) * NZ for k in range(2)]
            at_home = at_home & (y // 2 == side)
        base_z = [lax.rem(me[2] + k, NZ) for k in range(NZ)]
        bases = [(x, y) for y in base_y for x in base_x]
        count = len(bases) * NZ
        for n in range(count):
            step = n * STRIDE % count
            x, y = bases[step % len(bases)]
            yield (at_home if step == 0 else None), x + y + base_z[step // len(bases)]

    def visit(planes, act, first=(), side=None):
        for there in first:
            pl.when(my_dev != there)(lambda: act(jnp.int32(there)))
        for self_at, there in members(planes, side):
            go = None if self_at is None else not_(self_at)
            for known in first:
                go = there != known if go is None else go & (there != known)
            if go is None:
                act(there)
            else:
                pl.when(go)(lambda: act(there))

    for load in loads:
        load.wait()
    weight[...] = volume[...] * jnp.exp(-LOG_STEP * exponent[...].astype(f32))
    y_layer[...] = weight[pl.ds(SPAN - 1, SPAN, stride=SPAN), :]
    last = one_hot(iota((8, LANES), 1) == LANES - 1)
    edge[...] = pick_t(last, weight[...])[0:1]

    @pl.when(is_root)
    def _():
        pl.semaphore_wait(barrier, DEV - 1)

    @pl.when(is_mid_root)
    def _():
        pl.semaphore_wait(barrier, DEV // 4 * 3 - 1)

    @pl.when(is_early_root)
    def _():
        pl.semaphore_wait(barrier, DEV // 2 - 1)

    @pl.when(not_(is_root | is_mid_root | is_early_root))
    def _():
        pl.semaphore_wait(barrier, len(HALO))

    halo_from = (
        weight.at[pl.ds(ROWS - SPAN, SPAN)], y_layer, weight.at[pl.ds(ROWS - 8, 8)],
        edge, edge, edge, edge,
    )
    halo_to = (
        lines_got.at[pl.ds(0, SPAN)], lines_got.at[pl.ds(SPAN, SPAN)],
        lines_got.at[pl.ds(2 * SPAN, 8)], *(z_got.at[n] for n in range(4)),
    )
    halos = []
    for n, step in enumerate(HALO):
        copy = pltpu.make_async_remote_copy(
            src_ref=halo_from[n], dst_ref=halo_to[n],
            send_sem=halo_send.at[n], recv_sem=halo_recv.at[n],
            device_id=ahead(*step), device_id_type=LOGICAL,
        )
        copy.start()
        halos.append(copy)

    @pl.when(is_early_root)
    def _():
        visit((0, 1), lambda there: signal(early_sem, there))

    @pl.when(is_mid_root)
    def _():
        visit((0, 1), lambda there: signal(mid_sem, there), FIRST)
        visit((2,), lambda there: signal(mid_sem, there))

    @pl.when(is_root)
    def _():
        visit((3,), lambda there: signal(go_sem, there))
        visit((0, 1), lambda there: signal(go_sem, there), FIRST)
        visit((2,), lambda there: signal(go_sem, there))

    owner_dev = owner[...] // ROWS
    slots = (owner[...] - owner_dev * ROWS).astype(f32)
    same = owner_dev == iota((DEV, ROWS), 0)
    before = one_hot(iota((ROWS, ROWS), 0) < iota((ROWS, ROWS), 1))
    rank = dot_n(one_hot(same), before)
    ranked = [one_hot(same & (rank == value)) for value in (0.0, 1.0)]
    order = jnp.concatenate(ranked, axis=0)

    def put(part, rows):
        packed[2 * part] = rows[:DEV]
        packed[2 * part + 1] = rows[DEV:]

    own = weight[...].reshape(SPAN, SPAN, LANES)
    put(0, pick(order, weight[...]))

    def send(first, count):
        def act(there):
            pltpu.make_async_remote_copy(
                src_ref=packed.at[pl.ds(first, count), pl.ds(there, 1), :],
                dst_ref=got.at[pl.ds(first, count), pl.ds(my_dev, 1), :],
                send_sem=send_sem, recv_sem=recv_sem,
                device_id=there, device_id_type=LOGICAL,
            ).start()

        return act

    @pl.when(is_early & not_(is_early_root))
    def _():
        pl.semaphore_wait(early_sem, 1)

    @pl.when(is_mid & not_(is_mid_root))
    def _():
        pl.semaphore_wait(mid_sem, 1)

    @pl.when(is_late & not_(is_root))
    def _():
        pl.semaphore_wait(go_sem, 1)

    visit((0, 1), send(0, 2))

    @pl.when(is_early)
    def _():
        pl.semaphore_wait(mid_sem, 1)

    visit((2,), send(0, 2))

    @pl.when(not_(is_late))
    def _():
        pl.semaphore_wait(go_sem, 1)

    visit((3,), send(0, 2))


    empty = jnp.zeros((1, SPAN, LANES), f32)
    behind_x = jnp.concatenate([empty, own[:-1]], axis=0)
    column = jnp.zeros((SPAN, 1, LANES), f32)
    behind_y = jnp.concatenate([column, own[:, :-1]], axis=1)
    behind_xy = jnp.concatenate([column, behind_x[:, :-1]], axis=1)
    from_row, line = iota((ROWS, LANES), 0), iota((ROWS, LANES), 1)
    in_x, in_y = line < SPAN, (line >= SPAN) & (line < 2 * SPAN)
    wanted = (
        jnp.where(in_x, line, -1),
        jnp.where(in_y, (line - SPAN) * SPAN, -1),
        jnp.where(
            in_x & (line < SPAN - 1),
            line + 1,
            jnp.where(
                in_y & (line < 2 * SPAN - 1),
                (line - SPAN + 1) * SPAN,
                jnp.where(line == 2 * SPAN + 7, 0, -1),
            ),
        ),
    )
    selects = []
    for n, inner in enumerate((behind_x, behind_y, behind_xy)):
        put(n + 1, pick(order, inner.reshape(ROWS, LANES)))
        selects.append(dot_n(order, one_hot(from_row == wanted[n])).astype(bf16))
    select = jnp.concatenate(selects, axis=0)

    for copy in halos:
        copy.wait()

    pad = jnp.zeros((LANES - 2 * SPAN - 8, LANES), f32)
    rim = pick(select, jnp.concatenate([lines_got[...], pad], axis=0))
    for n in range(6):
        packed[n + 2] += rim[n * DEV : (n + 1) * DEV]

    at = iota((1, ROWS), 1)
    first_x, first_y = at < SPAN, at % SPAN == 0
    z_own, z_x, z_y, z_xy = (z_got[n] for n in range(4))

    def turn(row, by):
        return pltpu.roll(row, by % ROWS, 1)

    z_rows = (
        z_own,
        jnp.where(first_x, turn(z_x, SPAN), turn(z_own, SPAN)),
        jnp.where(first_y, turn(z_y, 1 - SPAN), turn(z_own, 1)),
        jnp.where(
            first_x,
            jnp.where(first_y, turn(z_xy, 1), turn(z_x, SPAN + 1)),
            jnp.where(first_y, turn(z_y, 1), turn(z_own, SPAN + 1)),
        ),
        slots,
    )
    table = jnp.zeros((8, ROWS), f32)
    for n, row in enumerate(z_rows):
        table = jnp.where(iota((8, ROWS), 0) == n, row, table)
    blank = jnp.zeros((LANES - 16, ROWS), f32)
    none = jnp.zeros((8, ROWS), f32)
    packed[8] = pick_t(ranked[0], jnp.concatenate([table, none, blank], axis=0)) + pick_t(
        ranked[1], jnp.concatenate([none, table, blank], axis=0)
    )

    keep = pltpu.make_async_copy(
        packed.at[:, pl.ds(my_dev, 1), :], got.at[:, pl.ds(my_dev, 1), :], own_sem
    )
    keep.start()
    visit((0, 1), send(2, PARTS - 2))

    visit((2,), send(2, PARTS - 2))

    visit((3,), send(2, PARTS - 2))
    keep.wait()
    all_others = pl.ds(0, DEV - 1)
    pltpu.make_async_remote_copy(
        src_ref=packed.at[:, all_others], dst_ref=got.at[:, all_others],
        send_sem=send_sem, recv_sem=recv_sem, device_id=my_dev, device_id_type=LOGICAL,
    ).wait()


def assemble(got, stencil_hbm, lumped_hbm, stencil, lumped, out_sems, lump_sem):
    rows = ROWS // CHUNKS
    extra = got[8]
    tails = [extra, pltpu.roll(extra, LANES - 8, 1)]
    slot = jnp.concatenate(
        [
            dot_t(one_hot(iota((8, LANES), 1) == 4), tail.astype(bf16))[0:1]
            for tail in tails
        ],
        axis=1,
    )
    five = [(got[2 * n], got[2 * n + 1]) for n in range(4)] + [tails]
    five = [jnp.concatenate(pieces(jnp.concatenate(two, axis=0)), axis=1) for two in five]
    lane = iota((rows, LANES), 1)
    copies = []
    for chunk in range(CHUNKS):
        here = pl.ds(chunk * rows, rows)
        mine = iota((rows, ROWS), 0) + chunk * rows
        place = one_hot(slot == mine.astype(f32), 0.015625)
        both = [dot_n(place, two) for two in five]
        placed = [pair[:, :LANES] + pair[:, LANES:] for pair in both]
        now, tail = placed[:4], placed[4]
        behind = [
            jnp.where(lane == 0, tail[:, n : n + 1], pltpu.roll(line, 1, 1))
            for n, line in enumerate(now)
        ]
        total = sum(now) + sum(behind)
        lumped[here, :] = 1.0 / (27.0 * total)

        def spread(current, back):
            return (back, 2.0 * (current + back), current)

        def plane(four):
            along = zip(spread(four[0], four[1]), spread(four[2], four[3]))
            return [value for current, back in along for value in spread(current, back)]

        for n, (current, back) in enumerate(zip(plane(now), plane(behind))):
            for k, value in enumerate(spread(current, back)):
                stencil[3 * n + k, here, :] = value
        copy = pltpu.make_async_copy(
            stencil.at[:, here], stencil_hbm.at[:, here], out_sems.at[chunk]
        )
        copy.start()
        copies.append(copy)
    copy = pltpu.make_async_copy(lumped, lumped_hbm, lump_sem)
    copy.start()
    copies.append(copy)
    for copy in copies:
        copy.wait()


def in_hbm(x):
    return pltpu.with_memory_space_constraint(x, pltpu.HBM)


def shards(cell_volume, exponent, owner_row):
    vmem = pl.BlockSpec(memory_space=pltpu.VMEM)
    hbm = pl.BlockSpec(memory_space=pltpu.HBM)
    dma, regular = pltpu.SemaphoreType.DMA, pltpu.SemaphoreType.REGULAR
    got = pl.pallas_call(
        exchange,
        name="exchange",
        out_shape=pltpu.VMEM((PARTS, DEV, LANES), f32),
        in_specs=[hbm] * 3,
        out_specs=vmem,
        scratch_shapes=[
            pltpu.VMEM((ROWS, LANES), f32),
            pltpu.VMEM((ROWS, LANES), i32),
            pltpu.VMEM((1, ROWS), i32),
            pltpu.VMEM((ROWS, LANES), f32),
            pltpu.VMEM((SPAN, LANES), f32),
            pltpu.VMEM((1, ROWS), f32),
            pltpu.VMEM((2 * SPAN + 8, LANES), f32),
            pltpu.VMEM((4, 1, ROWS), f32),
            pltpu.VMEM((PARTS, DEV, LANES), f32),
            dma((3,)), dma((7,)), dma((7,)), dma, dma, dma, regular, regular, regular,
        ],
        compiler_params=pltpu.CompilerParams(
            has_side_effects=True, collective_id=1, vmem_limit_bytes=16 << 20
        ),
    )(
        in_hbm(cell_volume.reshape(ROWS, LANES)),
        in_hbm(exponent.reshape(ROWS, LANES)),
        in_hbm(owner_row.reshape(1, ROWS)),
    )
    return pl.pallas_call(
        assemble,
        name="assemble",
        out_shape=(
            jax.ShapeDtypeStruct((27, ROWS, LANES), f32),
            jax.ShapeDtypeStruct((ROWS, LANES), f32),
        ),
        in_specs=[vmem],
        out_specs=(hbm, hbm),
        scratch_shapes=[
            pltpu.VMEM((27, ROWS, LANES), f32),
            pltpu.VMEM((ROWS, LANES), f32),
            dma((CHUNKS,)), dma,
        ],
        compiler_params=pltpu.CompilerParams(vmem_limit_bytes=16 << 20),
    )(got)


def solution(mesh):
    return jax.shard_map(
        shards,
        mesh=mesh,
        in_specs=(P(*AXES), P(*AXES), P(AXES)),
        out_specs=(P(None, AXES, None), P(AXES, None)),
        check_vma=False,
    )
```

```python
import jax
import jax.numpy as jnp
from jax import lax
from jax.experimental import pallas as pl
from jax.experimental.pallas import tpu as pltpu
from jax.sharding import PartitionSpec as P

LOGICAL = pl.DeviceIdType.LOGICAL
AXES = ("gx", "gy", "gz")
LOG_STEP = 0.3
NX, NY, NZ = 4, 8, 4
DEV = NX * NY * NZ
HALF = NY // 2
PLANES = 4
ROOT = (3 * NY + 6) * NZ + 2
EARLY_ROOT = (3 * NY + 2) * NZ + 2
MID_ROOT = (0 * NY + 6) * NZ + 2
FIRST = (NY * NZ, 0)
SPAN = 16
ROWS = SPAN * SPAN
LANES = 128
PARTS = 9
STRIDE = 13
CHUNKS = 4
HALO = ((1, 0, 0), (0, 1, 0), (1, 1, 0), (0, 0, 1), (1, 0, 1), (0, 1, 1), (1, 1, 1))

f32, bf16, i32 = jnp.float32, jnp.bfloat16, jnp.int32


def pieces(x):
    high = x.astype(bf16)
    return high, (x - high.astype(f32)).astype(bf16)


def dot_t(a, b):
    return lax.dot_general(a, b, (((1,), (1,)), ((), ())), preferred_element_type=f32)


def dot_n(a, b):
    return lax.dot_general(a, b, (((1,), (0,)), ((), ())), preferred_element_type=f32)


def pick(select, x):
    both = dot_n(select, jnp.concatenate(pieces(x), axis=1))
    return both[:, :LANES] + both[:, LANES:]


def pick_t(select, x):
    return sum(dot_t(select, piece) for piece in pieces(x))


def iota(shape, axis):
    return lax.broadcasted_iota(i32, shape, axis)


def one_hot(mask, value=1.0):
    return jnp.where(mask, value, 0.0).astype(bf16)


def exchange(
    volume_hbm, exponent_hbm, owner_hbm, got,
    volume, exponent, owner, weight, y_layer, edge,
    lines_got, z_got, packed,
    in_sems, halo_send, halo_recv, send_sem, recv_sem, own_sem, go_sem, mid_sem, early_sem,
):
    loads = [
        pltpu.make_async_copy(src, dst, in_sems.at[n])
        for n, (src, dst) in enumerate(
            ((volume_hbm, volume), (exponent_hbm, exponent), (owner_hbm, owner))
        )
    ]
    for load in loads:
        load.start()

    me = tuple(lax.axis_index(axis) for axis in AXES)
    my_dev = (me[0] * NY + me[1]) * NZ + me[2]
    is_root, is_mid_root, is_early_root = (
        my_dev == root for root in (ROOT, MID_ROOT, EARLY_ROOT)
    )
    my_plane = me[0] // 2 + 2 * (me[1] // HALF)
    is_early, is_mid, is_late = my_plane < 2, my_plane == 2, my_plane == 3
    not_ = jnp.logical_not

    def ahead(x, y, z):
        there_x = lax.rem(me[0] + x % NX, NX)
        there_y = lax.rem(me[1] + y % NY, NY)
        there_z = lax.rem(me[2] + z % NZ, NZ)
        return (there_x * NY + there_y) * NZ + there_z

    def signal(sem, there):
        pl.semaphore_signal(sem, inc=1, device_id=there, device_id_type=LOGICAL)

    barrier = pltpu.get_barrier_semaphore()
    sources = [ahead(-x, -y, -z) for x, y, z in HALO]
    def greet(root, wanted):
        known = sum((source == root).astype(i32) for source in sources)

        @pl.when(wanted & (my_dev != root) & (known == 0))
        def _():
            signal(barrier, jnp.int32(root))

    greet(ROOT, my_dev >= 0)
    greet(MID_ROOT, not_(is_late))
    greet(EARLY_ROOT, is_early)
    for source in sources:
        signal(barrier, source)

    def members(planes, side=None):
        z_hi, z_lo = planes[0] // 2, planes[0] % 2
        core, y = lax.rem(me[0], 2), lax.rem(me[1], HALF)
        if len(planes) == 2:
            base_x = [lax.rem(me[0] + k, NX) * (NY * NZ) for k in range(NX)]
            at_home = me[1] // HALF == z_hi
        else:
            base_x = [(z_lo * 2 + lax.rem(core + k, 2)) * (NY * NZ) for k in range(2)]
            at_home = my_plane == planes[0]
        if side is None:
            base_y = [(z_hi * HALF + lax.rem(y + k, HALF)) * NZ for k in range(HALF)]
        else:
            base_y = [(z_hi * HALF + side * 2 + lax.rem(y + k, 2)) * NZ for k in range(2)]
            at_home = at_home & (y // 2 == side)
        base_z = [lax.rem(me[2] + k, NZ) for k in range(NZ)]
        bases = [(x, y) for y in base_y for x in base_x]
        count = len(bases) * NZ
        for n in range(count):
            step = n * STRIDE % count
            x, y = bases[step % len(bases)]
            yield (at_home if step == 0 else None), x + y + base_z[step // len(bases)]

    def visit(planes, act, first=(), side=None):
        for there in first:
            pl.when(my_dev != there)(lambda: act(jnp.int32(there)))
        for self_at, there in members(planes, side):
            go = None if self_at is None else not_(self_at)
            for known in first:
                go = there != known if go is None else go & (there != known)
            if go is None:
                act(there)
            else:
                pl.when(go)(lambda: act(there))

    for load in loads:
        load.wait()
    weight[...] = volume[...] * jnp.exp(-LOG_STEP * exponent[...].astype(f32))
    y_layer[...] = weight[pl.ds(SPAN - 1, SPAN, stride=SPAN), :]
    last = one_hot(iota((8, LANES), 1) == LANES - 1)
    edge[...] = pick_t(last, weight[...])[0:1]

    @pl.when(is_root)
    def _():
        pl.semaphore_wait(barrier, DEV - 1)

    @pl.when(is_mid_root)
    def _():
        pl.semaphore_wait(barrier, DEV // 4 * 3 - 1)

    @pl.when(is_early_root)
    def _():
        pl.semaphore_wait(barrier, DEV // 2 - 1)

    @pl.when(not_(is_root | is_mid_root | is_early_root))
    def _():
        pl.semaphore_wait(barrier, len(HALO))

    halo_from = (
        weight.at[pl.ds(ROWS - SPAN, SPAN)], y_layer, weight.at[pl.ds(ROWS - 8, 8)],
        edge, edge, edge, edge,
    )
    halo_to = (
        lines_got.at[pl.ds(0, SPAN)], lines_got.at[pl.ds(SPAN, SPAN)],
        lines_got.at[pl.ds(2 * SPAN, 8)], *(z_got.at[n] for n in range(4)),
    )
    halos = []
    for n, step in enumerate(HALO):
        copy = pltpu.make_async_remote_copy(
            src_ref=halo_from[n], dst_ref=halo_to[n],
            send_sem=halo_send.at[n], recv_sem=halo_recv.at[n],
            device_id=ahead(*step), device_id_type=LOGICAL,
        )
        copy.start()
        halos.append(copy)

    @pl.when(is_early_root)
    def _():
        visit((0, 1), lambda there: signal(early_sem, there))

    @pl.when(is_mid_root)
    def _():
        visit((0, 1), lambda there: signal(mid_sem, there), FIRST)
        visit((2,), lambda there: signal(mid_sem, there))

    @pl.when(is_root)
    def _():
        visit((3,), lambda there: signal(go_sem, there))
        visit((0, 1), lambda there: signal(go_sem, there), FIRST)
        visit((2,), lambda there: signal(go_sem, there))

    owner_dev = owner[...] // ROWS
    slots = (owner[...] - owner_dev * ROWS).astype(f32)
    same = owner_dev == iota((DEV, ROWS), 0)
    before = one_hot(iota((ROWS, ROWS), 0) < iota((ROWS, ROWS), 1))
    rank = dot_n(one_hot(same), before)
    ranked = [one_hot(same & (rank == value)) for value in (0.0, 1.0)]
    order = jnp.concatenate(ranked, axis=0)

    def put(part, rows):
        packed[2 * part] = rows[:DEV]
        packed[2 * part + 1] = rows[DEV:]

    own = weight[...].reshape(SPAN, SPAN, LANES)
    put(0, pick(order, weight[...]))

    def send(first, count):
        def act(there):
            pltpu.make_async_remote_copy(
                src_ref=packed.at[pl.ds(first, count), pl.ds(there, 1), :],
                dst_ref=got.at[pl.ds(first, count), pl.ds(my_dev, 1), :],
                send_sem=send_sem, recv_sem=recv_sem,
                device_id=there, device_id_type=LOGICAL,
            ).start()

        return act

    empty = jnp.zeros((1, SPAN, LANES), f32)
    behind_x = jnp.concatenate([empty, own[:-1]], axis=0)
    column = jnp.zeros((SPAN, 1, LANES), f32)
    behind_y = jnp.concatenate([column, own[:, :-1]], axis=1)
    behind_xy = jnp.concatenate([column, behind_x[:, :-1]], axis=1)
    from_row, line = iota((ROWS, LANES), 0), iota((ROWS, LANES), 1)
    in_x, in_y = line < SPAN, (line >= SPAN) & (line < 2 * SPAN)
    wanted = (
        jnp.where(in_x, line, -1),
        jnp.where(in_y, (line - SPAN) * SPAN, -1),
        jnp.where(
            in_x & (line < SPAN - 1),
            line + 1,
            jnp.where(
                in_y & (line < 2 * SPAN - 1),
                (line - SPAN + 1) * SPAN,
                jnp.where(line == 2 * SPAN + 7, 0, -1),
            ),
        ),
    )
    selects = []
    for n, inner in enumerate((behind_x, behind_y, behind_xy)):
        put(n + 1, pick(order, inner.reshape(ROWS, LANES)))
        selects.append(dot_n(order, one_hot(from_row == wanted[n])).astype(bf16))
    select = jnp.concatenate(selects, axis=0)
    select = jnp.concatenate([select, select], axis=1)

    halos[0].wait()
    pad = jnp.zeros((LANES - SPAN, LANES), f32)
    x_lines = jnp.concatenate([lines_got[0:SPAN], pad], axis=0)
    rim = dot_n(select[:ROWS], jnp.concatenate(pieces(x_lines), axis=0))
    for n in range(2):
        packed[n + 2] += rim[n * DEV : (n + 1) * DEV]

    @pl.when(is_early & not_(is_early_root))
    def _():
        pl.semaphore_wait(early_sem, 1)

    @pl.when(is_mid & not_(is_mid_root))
    def _():
        pl.semaphore_wait(mid_sem, 1)

    @pl.when(is_late & not_(is_root))
    def _():
        pl.semaphore_wait(go_sem, 1)

    visit((0, 1), send(0, 4))

    @pl.when(is_early & not_(is_mid_root))
    def _():
        pl.semaphore_wait(mid_sem, 1)

    visit((2,), send(0, 4))

    @pl.when(not_(is_late))
    def _():
        pl.semaphore_wait(go_sem, 1)

    visit((3,), send(0, 4))


    for copy in halos[1:]:
        copy.wait()

    pad = jnp.zeros((LANES - 2 * SPAN - 8, LANES), f32)
    rim_lines = jnp.concatenate([lines_got[...], pad], axis=0)
    rim = dot_n(select[ROWS:], jnp.concatenate(pieces(rim_lines), axis=0))
    for n in range(4):
        packed[n + 4] += rim[n * DEV : (n + 1) * DEV]

    at = iota((1, ROWS), 1)
    first_x, first_y = at < SPAN, at % SPAN == 0
    z_own, z_x, z_y, z_xy = (z_got[n] for n in range(4))

    def turn(row, by):
        return pltpu.roll(row, by % ROWS, 1)

    z_rows = (
        z_own,
        jnp.where(first_x, turn(z_x, SPAN), turn(z_own, SPAN)),
        jnp.where(first_y, turn(z_y, 1 - SPAN), turn(z_own, 1)),
        jnp.where(
            first_x,
            jnp.where(first_y, turn(z_xy, 1), turn(z_x, SPAN + 1)),
            jnp.where(first_y, turn(z_y, 1), turn(z_own, SPAN + 1)),
        ),
        slots,
    )
    table = jnp.zeros((8, ROWS), f32)
    for n, row in enumerate(z_rows):
        table = jnp.where(iota((8, ROWS), 0) == n, row, table)
    high, low = pieces(table)
    none = jnp.zeros((16, ROWS), bf16)
    blank = jnp.zeros((LANES - 32, ROWS), bf16)
    both = jnp.concatenate([high, low], axis=0)
    packed[8] = dot_t(ranked[0], jnp.concatenate([both, none, blank], axis=0)) + dot_t(
        ranked[1], jnp.concatenate([none, both, blank], axis=0)
    )

    keep = pltpu.make_async_copy(
        packed.at[:, pl.ds(my_dev, 1), :], got.at[:, pl.ds(my_dev, 1), :], own_sem
    )
    keep.start()
    visit((0, 1), send(4, PARTS - 4), FIRST)

    visit((2,), send(4, PARTS - 4))

    visit((3,), send(4, PARTS - 4))
    keep.wait()
    all_others = pl.ds(0, DEV - 1)
    pltpu.make_async_remote_copy(
        src_ref=packed.at[:, all_others], dst_ref=got.at[:, all_others],
        send_sem=send_sem, recv_sem=recv_sem, device_id=my_dev, device_id_type=LOGICAL,
    ).wait()


def assemble(got, stencil_hbm, lumped_hbm, stencil, lumped, out_sems, lump_sem):
    rows = ROWS // CHUNKS
    extra = got[8]
    extra += pltpu.roll(extra, LANES - 8, 1)
    tails = [extra, pltpu.roll(extra, LANES - 16, 1)]
    slot = jnp.concatenate(
        [
            dot_t(one_hot(iota((8, LANES), 1) == 4), tail.astype(bf16))[0:1]
            for tail in tails
        ],
        axis=1,
    )
    five = [(got[2 * n], got[2 * n + 1]) for n in range(4)] + [tails]
    five = [jnp.concatenate(pieces(jnp.concatenate(two, axis=0)), axis=1) for two in five]
    lane = iota((rows, LANES), 1)
    copies = []
    for chunk in range(CHUNKS):
        here = pl.ds(chunk * rows, rows)
        mine = iota((rows, ROWS), 0) + chunk * rows
        place = one_hot(slot == mine.astype(f32), 0.015625)
        both = [dot_n(place, two) for two in five]
        placed = [pair[:, :LANES] + pair[:, LANES:] for pair in both]
        now, tail = placed[:4], placed[4]
        behind = [
            jnp.where(lane == 0, tail[:, n : n + 1], pltpu.roll(line, 1, 1))
            for n, line in enumerate(now)
        ]
        total = sum(now) + sum(behind)
        lumped[here, :] = 1.0 / (27.0 * total)

        def spread(current, back):
            return (back, 2.0 * (current + back), current)

        def plane(four):
            along = zip(spread(four[0], four[1]), spread(four[2], four[3]))
            return [value for current, back in along for value in spread(current, back)]

        for n, (current, back) in enumerate(zip(plane(now), plane(behind))):
            for k, value in enumerate(spread(current, back)):
                stencil[3 * n + k, here, :] = value
        copy = pltpu.make_async_copy(
            stencil.at[:, here], stencil_hbm.at[:, here], out_sems.at[chunk]
        )
        copy.start()
        copies.append(copy)
    copy = pltpu.make_async_copy(lumped, lumped_hbm, lump_sem)
    copy.start()
    copies.append(copy)
    for copy in copies:
        copy.wait()


def in_hbm(x):
    return pltpu.with_memory_space_constraint(x, pltpu.HBM)


def shards(cell_volume, exponent, owner_row):
    vmem = pl.BlockSpec(memory_space=pltpu.VMEM)
    hbm = pl.BlockSpec(memory_space=pltpu.HBM)
    dma, regular = pltpu.SemaphoreType.DMA, pltpu.SemaphoreType.REGULAR
    got = pl.pallas_call(
        exchange,
        name="exchange",
        out_shape=pltpu.VMEM((PARTS, DEV, LANES), f32),
        in_specs=[hbm] * 3,
        out_specs=vmem,
        scratch_shapes=[
            pltpu.VMEM((ROWS, LANES), f32),
            pltpu.VMEM((ROWS, LANES), i32),
            pltpu.VMEM((1, ROWS), i32),
            pltpu.VMEM((ROWS, LANES), f32),
            pltpu.VMEM((SPAN, LANES), f32),
            pltpu.VMEM((1, ROWS), f32),
            pltpu.VMEM((2 * SPAN + 8, LANES), f32),
            pltpu.VMEM((4, 1, ROWS), f32),
            pltpu.VMEM((PARTS, DEV, LANES), f32),
            dma((3,)), dma((7,)), dma((7,)), dma, dma, dma, regular, regular, regular,
        ],
        compiler_params=pltpu.CompilerParams(
            has_side_effects=True, collective_id=1, vmem_limit_bytes=16 << 20
        ),
    )(
        in_hbm(cell_volume.reshape(ROWS, LANES)),
        in_hbm(exponent.reshape(ROWS, LANES)),
        in_hbm(owner_row.reshape(1, ROWS)),
    )
    return pl.pallas_call(
        assemble,
        name="assemble",
        out_shape=(
            jax.ShapeDtypeStruct((27, ROWS, LANES), f32),
            jax.ShapeDtypeStruct((ROWS, LANES), f32),
        ),
        in_specs=[vmem],
        out_specs=(hbm, hbm),
        scratch_shapes=[
            pltpu.VMEM((27, ROWS, LANES), f32),
            pltpu.VMEM((ROWS, LANES), f32),
            dma((CHUNKS,)), dma,
        ],
        compiler_params=pltpu.CompilerParams(vmem_limit_bytes=16 << 20),
    )(got)


def solution(mesh):
    return jax.shard_map(
        shards,
        mesh=mesh,
        in_specs=(P(*AXES), P(*AXES), P(AXES)),
        out_specs=(P(None, AXES, None), P(AXES, None)),
        check_vma=False,
    )
```

```python
import jax
import jax.numpy as jnp
from jax import lax
from jax.experimental import pallas as pl
from jax.experimental.pallas import tpu as pltpu
from jax.sharding import PartitionSpec as P

LOGICAL = pl.DeviceIdType.LOGICAL
AXES = ("gx", "gy", "gz")
LOG_STEP = 0.3
NX, NY, NZ = 4, 8, 4
DEV = NX * NY * NZ
HALF = NY // 2
PLANES = 4
ROOT = (3 * NY + 6) * NZ + 2
EARLY_ROOT = (3 * NY + 2) * NZ + 2
MID_ROOT = (0 * NY + 6) * NZ + 2
FIRST = (NY * NZ, 0)
SPAN = 16
ROWS = SPAN * SPAN
LANES = 128
PARTS = 9
STRIDE = 13
CHUNKS = 4
HALO = ((1, 0, 0), (0, 1, 0), (1, 1, 0), (0, 0, 1), (1, 0, 1), (0, 1, 1), (1, 1, 1))

f32, bf16, i32 = jnp.float32, jnp.bfloat16, jnp.int32


def pieces(x):
    high = x.astype(bf16)
    return high, (x - high.astype(f32)).astype(bf16)


def dot_t(a, b):
    return lax.dot_general(a, b, (((1,), (1,)), ((), ())), preferred_element_type=f32)


def dot_n(a, b):
    return lax.dot_general(a, b, (((1,), (0,)), ((), ())), preferred_element_type=f32)


def pick(select, x):
    both = dot_n(select, jnp.concatenate(pieces(x), axis=1))
    return both[:, :LANES] + both[:, LANES:]


def pick_t(select, x):
    return sum(dot_t(select, piece) for piece in pieces(x))


def iota(shape, axis):
    return lax.broadcasted_iota(i32, shape, axis)


def one_hot(mask, value=1.0):
    return jnp.where(mask, value, 0.0).astype(bf16)


def exchange(
    volume_hbm, exponent_hbm, owner_hbm, got,
    volume, exponent, owner, weight, y_layer, edge,
    lines_got, z_got, packed,
    in_sems, halo_send, halo_recv, send_sem, recv_sem, own_sem, go_sem, mid_sem, early_sem,
):
    loads = [
        pltpu.make_async_copy(src, dst, in_sems.at[n])
        for n, (src, dst) in enumerate(
            ((volume_hbm, volume), (exponent_hbm, exponent), (owner_hbm, owner))
        )
    ]
    for load in loads:
        load.start()

    me = tuple(lax.axis_index(axis) for axis in AXES)
    my_dev = (me[0] * NY + me[1]) * NZ + me[2]
    is_root, is_mid_root, is_early_root = (
        my_dev == root for root in (ROOT, MID_ROOT, EARLY_ROOT)
    )
    my_plane = me[0] // 2 + 2 * (me[1] // HALF)
    is_early, is_mid, is_late = my_plane < 2, my_plane == 2, my_plane == 3
    not_ = jnp.logical_not

    def ahead(x, y, z):
        there_x = lax.rem(me[0] + x % NX, NX)
        there_y = lax.rem(me[1] + y % NY, NY)
        there_z = lax.rem(me[2] + z % NZ, NZ)
        return (there_x * NY + there_y) * NZ + there_z

    def signal(sem, there):
        pl.semaphore_signal(sem, inc=1, device_id=there, device_id_type=LOGICAL)

    barrier = pltpu.get_barrier_semaphore()
    sources = [ahead(-x, -y, -z) for x, y, z in HALO]
    def greet(root, wanted):
        known = sum((source == root).astype(i32) for source in sources)

        @pl.when(wanted & (my_dev != root) & (known == 0))
        def _():
            signal(barrier, jnp.int32(root))

    greet(ROOT, my_dev >= 0)
    greet(MID_ROOT, not_(is_late))
    greet(EARLY_ROOT, is_early)
    for source in sources:
        signal(barrier, source)

    def members(planes, side=None):
        z_hi, z_lo = planes[0] // 2, planes[0] % 2
        core, y = lax.rem(me[0], 2), lax.rem(me[1], HALF)
        if len(planes) == 2:
            base_x = [lax.rem(me[0] + k, NX) * (NY * NZ) for k in range(NX)]
            at_home = me[1] // HALF == z_hi
        else:
            base_x = [(z_lo * 2 + lax.rem(core + k, 2)) * (NY * NZ) for k in range(2)]
            at_home = my_plane == planes[0]
        if side is None:
            base_y = [(z_hi * HALF + lax.rem(y + k, HALF)) * NZ for k in range(HALF)]
        else:
            base_y = [(z_hi * HALF + side * 2 + lax.rem(y + k, 2)) * NZ for k in range(2)]
            at_home = at_home & (y // 2 == side)
        base_z = [lax.rem(me[2] + k, NZ) for k in range(NZ)]
        bases = [(x, y) for y in base_y for x in base_x]
        count = len(bases) * NZ
        for n in range(count):
            step = n * STRIDE % count
            x, y = bases[step % len(bases)]
            yield (at_home if step == 0 else None), x + y + base_z[step // len(bases)]

    def visit(planes, act, first=(), side=None):
        for there in first:
            pl.when(my_dev != there)(lambda: act(jnp.int32(there)))
        for self_at, there in members(planes, side):
            go = None if self_at is None else not_(self_at)
            for known in first:
                go = there != known if go is None else go & (there != known)
            if go is None:
                act(there)
            else:
                pl.when(go)(lambda: act(there))

    for load in loads:
        load.wait()
    weight[...] = volume[...] * jnp.exp(-LOG_STEP * exponent[...].astype(f32))
    y_layer[...] = weight[pl.ds(SPAN - 1, SPAN, stride=SPAN), :]
    last = one_hot(iota((8, LANES), 1) == LANES - 1)
    edge[...] = pick_t(last, weight[...])[0:1]

    @pl.when(is_root)
    def _():
        pl.semaphore_wait(barrier, DEV - 1)

    @pl.when(is_mid_root)
    def _():
        pl.semaphore_wait(barrier, DEV // 4 * 3 - 1)

    @pl.when(is_early_root)
    def _():
        pl.semaphore_wait(barrier, DEV // 2 - 1)

    @pl.when(not_(is_root | is_mid_root | is_early_root))
    def _():
        pl.semaphore_wait(barrier, len(HALO))

    halo_from = (
        weight.at[pl.ds(ROWS - SPAN, SPAN)], y_layer, weight.at[pl.ds(ROWS - 8, 8)],
        edge, edge, edge, edge,
    )
    halo_to = (
        lines_got.at[pl.ds(0, SPAN)], lines_got.at[pl.ds(SPAN, SPAN)],
        lines_got.at[pl.ds(2 * SPAN, 8)], *(z_got.at[n] for n in range(4)),
    )
    halos = []
    for n, step in enumerate(HALO):
        copy = pltpu.make_async_remote_copy(
            src_ref=halo_from[n], dst_ref=halo_to[n],
            send_sem=halo_send.at[n], recv_sem=halo_recv.at[n],
            device_id=ahead(*step), device_id_type=LOGICAL,
        )
        copy.start()
        halos.append(copy)

    @pl.when(is_early_root)
    def _():
        visit((0, 1), lambda there: signal(early_sem, there))

    @pl.when(is_mid_root)
    def _():
        visit((0, 1), lambda there: signal(mid_sem, there), FIRST)
        visit((2,), lambda there: signal(mid_sem, there))

    @pl.when(is_root)
    def _():
        visit((3,), lambda there: signal(go_sem, there))
        visit((0, 1), lambda there: signal(go_sem, there), FIRST)
        visit((2,), lambda there: signal(go_sem, there))

    owner_dev = owner[...] // ROWS
    slots = (owner[...] - owner_dev * ROWS).astype(f32)
    same = owner_dev == iota((DEV, ROWS), 0)
    before = one_hot(iota((ROWS, ROWS), 0) < iota((ROWS, ROWS), 1))
    rank = dot_n(one_hot(same), before)
    ranked = [one_hot(same & (rank == value)) for value in (0.0, 1.0)]
    order = jnp.concatenate(ranked, axis=0)

    def put(part, rows):
        packed[2 * part] = rows[:DEV]
        packed[2 * part + 1] = rows[DEV:]

    own = weight[...].reshape(SPAN, SPAN, LANES)
    put(0, pick(order, weight[...]))

    def send(first, count):
        def act(there):
            pltpu.make_async_remote_copy(
                src_ref=packed.at[pl.ds(first, count), pl.ds(there, 1), :],
                dst_ref=got.at[pl.ds(first, count), pl.ds(my_dev, 1), :],
                send_sem=send_sem, recv_sem=recv_sem,
                device_id=there, device_id_type=LOGICAL,
            ).start()

        return act

    empty = jnp.zeros((1, SPAN, LANES), f32)
    behind_x = jnp.concatenate([empty, own[:-1]], axis=0)
    column = jnp.zeros((SPAN, 1, LANES), f32)
    behind_y = jnp.concatenate([column, own[:, :-1]], axis=1)
    behind_xy = jnp.concatenate([column, behind_x[:, :-1]], axis=1)
    from_row, line = iota((ROWS, LANES), 0), iota((ROWS, LANES), 1)
    in_x, in_y = line < SPAN, (line >= SPAN) & (line < 2 * SPAN)
    wanted = (
        jnp.where(in_x, line, -1),
        jnp.where(in_y, (line - SPAN) * SPAN, -1),
        jnp.where(
            in_x & (line < SPAN - 1),
            line + 1,
            jnp.where(
                in_y & (line < 2 * SPAN - 1),
                (line - SPAN + 1) * SPAN,
                jnp.where(line == 2 * SPAN + 7, 0, -1),
            ),
        ),
    )
    selects = []
    for n, inner in enumerate((behind_x, behind_y, behind_xy)):
        put(n + 1, pick(order, inner.reshape(ROWS, LANES)))
        selects.append(dot_n(order, one_hot(from_row == wanted[n])).astype(bf16))
    select = jnp.concatenate(selects, axis=0)
    select = jnp.concatenate([select, select], axis=1)

    halos[0].wait()
    pad = jnp.zeros((LANES - SPAN, LANES), f32)
    x_lines = jnp.concatenate([lines_got[0:SPAN], pad], axis=0)
    rim = dot_n(select[:ROWS], jnp.concatenate(pieces(x_lines), axis=0))
    for n in range(2):
        packed[n + 2] += rim[n * DEV : (n + 1) * DEV]

    @pl.when(is_early & not_(is_early_root))
    def _():
        pl.semaphore_wait(early_sem, 1)

    @pl.when(is_mid & not_(is_mid_root))
    def _():
        pl.semaphore_wait(mid_sem, 1)

    @pl.when(is_late & not_(is_root))
    def _():
        pl.semaphore_wait(go_sem, 1)

    visit((0, 1), send(0, 4), FIRST)

    @pl.when(is_early & not_(is_mid_root))
    def _():
        pl.semaphore_wait(mid_sem, 1)

    visit((2,), send(0, 4))

    @pl.when(not_(is_late))
    def _():
        pl.semaphore_wait(go_sem, 1)

    visit((3,), send(0, 4))


    for copy in halos[1:]:
        copy.wait()

    pad = jnp.zeros((LANES - 2 * SPAN - 8, LANES), f32)
    rim_lines = jnp.concatenate([lines_got[...], pad], axis=0)
    rim = dot_n(select[ROWS:], jnp.concatenate(pieces(rim_lines), axis=0))
    for n in range(4):
        packed[n + 4] += rim[n * DEV : (n + 1) * DEV]

    at = iota((1, ROWS), 1)
    first_x, first_y = at < SPAN, at % SPAN == 0
    z_own, z_x, z_y, z_xy = (z_got[n] for n in range(4))

    def turn(row, by):
        return pltpu.roll(row, by % ROWS, 1)

    z_rows = (
        z_own,
        jnp.where(first_x, turn(z_x, SPAN), turn(z_own, SPAN)),
        jnp.where(first_y, turn(z_y, 1 - SPAN), turn(z_own, 1)),
        jnp.where(
            first_x,
            jnp.where(first_y, turn(z_xy, 1), turn(z_x, SPAN + 1)),
            jnp.where(first_y, turn(z_y, 1), turn(z_own, SPAN + 1)),
        ),
        slots,
    )
    table = jnp.zeros((8, ROWS), f32)
    for n, row in enumerate(z_rows):
        table = jnp.where(iota((8, ROWS), 0) == n, row, table)
    high, low = pieces(table)
    none = jnp.zeros((16, ROWS), bf16)
    blank = jnp.zeros((LANES - 32, ROWS), bf16)
    both = jnp.concatenate([high, low], axis=0)
    packed[8] = dot_t(ranked[0], jnp.concatenate([both, none, blank], axis=0)) + dot_t(
        ranked[1], jnp.concatenate([none, both, blank], axis=0)
    )

    keep = pltpu.make_async_copy(
        packed.at[:, pl.ds(my_dev, 1), :], got.at[:, pl.ds(my_dev, 1), :], own_sem
    )
    keep.start()
    visit((0, 1), send(4, PARTS - 4), FIRST)

    visit((2,), send(4, PARTS - 4))

    visit((3,), send(4, PARTS - 4))
    keep.wait()
    all_others = pl.ds(0, DEV - 1)
    pltpu.make_async_remote_copy(
        src_ref=packed.at[:, all_others], dst_ref=got.at[:, all_others],
        send_sem=send_sem, recv_sem=recv_sem, device_id=my_dev, device_id_type=LOGICAL,
    ).wait()


def assemble(got, stencil_hbm, lumped_hbm, stencil, lumped, out_sems, lump_sem):
    rows = ROWS // CHUNKS
    extra = got[8]
    extra += pltpu.roll(extra, LANES - 8, 1)
    tails = [extra, pltpu.roll(extra, LANES - 16, 1)]
    slot = jnp.concatenate(
        [
            dot_t(one_hot(iota((8, LANES), 1) == 4), tail.astype(bf16))[0:1]
            for tail in tails
        ],
        axis=1,
    )
    five = [(got[2 * n], got[2 * n + 1]) for n in range(4)] + [tails]
    five = [jnp.concatenate(pieces(jnp.concatenate(two, axis=0)), axis=1) for two in five]
    lane = iota((rows, LANES), 1)
    copies = []
    for chunk in range(CHUNKS):
        here = pl.ds(chunk * rows, rows)
        mine = iota((rows, ROWS), 0) + chunk * rows
        place = one_hot(slot == mine.astype(f32), 0.015625)
        both = [dot_n(place, two) for two in five]
        placed = [pair[:, :LANES] + pair[:, LANES:] for pair in both]
        now, tail = placed[:4], placed[4]
        behind = [
            jnp.where(lane == 0, tail[:, n : n + 1], pltpu.roll(line, 1, 1))
            for n, line in enumerate(now)
        ]
        total = sum(now) + sum(behind)
        lumped[here, :] = 1.0 / (27.0 * total)

        def spread(current, back):
            return (back, 2.0 * (current + back), current)

        def plane(four):
            along = zip(spread(four[0], four[1]), spread(four[2], four[3]))
            return [value for current, back in along for value in spread(current, back)]

        for n, (current, back) in enumerate(zip(plane(now), plane(behind))):
            for k, value in enumerate(spread(current, back)):
                stencil[3 * n + k, here, :] = value
        copy = pltpu.make_async_copy(
            stencil.at[:, here], stencil_hbm.at[:, here], out_sems.at[chunk]
        )
        copy.start()
        copies.append(copy)
    copy = pltpu.make_async_copy(lumped, lumped_hbm, lump_sem)
    copy.start()
    copies.append(copy)
    for copy in copies:
        copy.wait()


def in_hbm(x):
    return pltpu.with_memory_space_constraint(x, pltpu.HBM)


def shards(cell_volume, exponent, owner_row):
    vmem = pl.BlockSpec(memory_space=pltpu.VMEM)
    hbm = pl.BlockSpec(memory_space=pltpu.HBM)
    dma, regular = pltpu.SemaphoreType.DMA, pltpu.SemaphoreType.REGULAR
    got = pl.pallas_call(
        exchange,
        name="exchange",
        out_shape=pltpu.VMEM((PARTS, DEV, LANES), f32),
        in_specs=[hbm] * 3,
        out_specs=vmem,
        scratch_shapes=[
            pltpu.VMEM((ROWS, LANES), f32),
            pltpu.VMEM((ROWS, LANES), i32),
            pltpu.VMEM((1, ROWS), i32),
            pltpu.VMEM((ROWS, LANES), f32),
            pltpu.VMEM((SPAN, LANES), f32),
            pltpu.VMEM((1, ROWS), f32),
            pltpu.VMEM((2 * SPAN + 8, LANES), f32),
            pltpu.VMEM((4, 1, ROWS), f32),
            pltpu.VMEM((PARTS, DEV, LANES), f32),
            dma((3,)), dma((7,)), dma((7,)), dma, dma, dma, regular, regular, regular,
        ],
        compiler_params=pltpu.CompilerParams(
            has_side_effects=True, collective_id=1, vmem_limit_bytes=16 << 20
        ),
    )(
        in_hbm(cell_volume.reshape(ROWS, LANES)),
        in_hbm(exponent.reshape(ROWS, LANES)),
        in_hbm(owner_row.reshape(1, ROWS)),
    )
    return pl.pallas_call(
        assemble,
        name="assemble",
        out_shape=(
            jax.ShapeDtypeStruct((27, ROWS, LANES), f32),
            jax.ShapeDtypeStruct((ROWS, LANES), f32),
        ),
        in_specs=[vmem],
        out_specs=(hbm, hbm),
        scratch_shapes=[
            pltpu.VMEM((27, ROWS, LANES), f32),
            pltpu.VMEM((ROWS, LANES), f32),
            dma((CHUNKS,)), dma,
        ],
        compiler_params=pltpu.CompilerParams(vmem_limit_bytes=16 << 20),
    )(got)


def solution(mesh):
    return jax.shard_map(
        shards,
        mesh=mesh,
        in_specs=(P(*AXES), P(*AXES), P(AXES)),
        out_specs=(P(None, AXES, None), P(AXES, None)),
        check_vma=False,
    )
```

```python
import jax
import jax.numpy as jnp
from jax import lax
from jax.experimental import pallas as pl
from jax.experimental.pallas import tpu as pltpu
from jax.sharding import PartitionSpec as P

LOGICAL = pl.DeviceIdType.LOGICAL
AXES = ("gx", "gy", "gz")
LOG_STEP = 0.3
NX, NY, NZ = 4, 8, 4
DEV = NX * NY * NZ
HALF = NY // 2
PLANES = 4
ROOT = (3 * NY + 6) * NZ + 2
EARLY_ROOT = (3 * NY + 2) * NZ + 2
MID_ROOT = (0 * NY + 6) * NZ + 2
FIRST = (NY * NZ, 0)
SPAN = 16
ROWS = SPAN * SPAN
LANES = 128
PARTS = 9
STRIDE = 19
CHUNKS = 4
HALO = ((1, 0, 0), (0, 1, 0), (1, 1, 0), (0, 0, 1), (1, 0, 1), (0, 1, 1), (1, 1, 1))

f32, bf16, i32 = jnp.float32, jnp.bfloat16, jnp.int32


def pieces(x):
    high = x.astype(bf16)
    return high, (x - high.astype(f32)).astype(bf16)


def dot_t(a, b):
    return lax.dot_general(a, b, (((1,), (1,)), ((), ())), preferred_element_type=f32)


def dot_n(a, b):
    return lax.dot_general(a, b, (((1,), (0,)), ((), ())), preferred_element_type=f32)


def pick(select, x):
    both = dot_n(select, jnp.concatenate(pieces(x), axis=1))
    return both[:, :LANES] + both[:, LANES:]


def pick_t(select, x):
    return sum(dot_t(select, piece) for piece in pieces(x))


def iota(shape, axis):
    return lax.broadcasted_iota(i32, shape, axis)


def one_hot(mask, value=1.0):
    return jnp.where(mask, value, 0.0).astype(bf16)


def exchange(
    volume_hbm, exponent_hbm, owner_hbm, got,
    volume, exponent, owner, weight, y_layer, edge,
    lines_got, z_got, packed,
    in_sems, halo_send, halo_recv, send_sem, recv_sem, own_sem, go_sem, mid_sem, early_sem,
):
    loads = [
        pltpu.make_async_copy(src, dst, in_sems.at[n])
        for n, (src, dst) in enumerate(
            ((volume_hbm, volume), (exponent_hbm, exponent), (owner_hbm, owner))
        )
    ]
    for load in loads:
        load.start()

    me = tuple(lax.axis_index(axis) for axis in AXES)
    my_dev = (me[0] * NY + me[1]) * NZ + me[2]
    is_root, is_mid_root, is_early_root = (
        my_dev == root for root in (ROOT, MID_ROOT, EARLY_ROOT)
    )
    my_plane = me[0] // 2 + 2 * (me[1] // HALF)
    is_early, is_mid, is_late = my_plane < 2, my_plane == 2, my_plane == 3
    not_ = jnp.logical_not

    def ahead(x, y, z):
        there_x = lax.rem(me[0] + x % NX, NX)
        there_y = lax.rem(me[1] + y % NY, NY)
        there_z = lax.rem(me[2] + z % NZ, NZ)
        return (there_x * NY + there_y) * NZ + there_z

    def signal(sem, there):
        pl.semaphore_signal(sem, inc=1, device_id=there, device_id_type=LOGICAL)

    barrier = pltpu.get_barrier_semaphore()
    sources = [ahead(-x, -y, -z) for x, y, z in HALO]
    def greet(root, wanted):
        known = sum((source == root).astype(i32) for source in sources)

        @pl.when(wanted & (my_dev != root) & (known == 0))
        def _():
            signal(barrier, jnp.int32(root))

    greet(ROOT, my_dev >= 0)
    greet(MID_ROOT, not_(is_late))
    greet(EARLY_ROOT, is_early)
    for source in sources:
        signal(barrier, source)

    def members(planes, side=None):
        z_hi, z_lo = planes[0] // 2, planes[0] % 2
        core, y = lax.rem(me[0], 2), lax.rem(me[1], HALF)
        if len(planes) == 2:
            base_x = [lax.rem(me[0] + k, NX) * (NY * NZ) for k in range(NX)]
            at_home = me[1] // HALF == z_hi
        else:
            base_x = [(z_lo * 2 + lax.rem(core + k, 2)) * (NY * NZ) for k in range(2)]
            at_home = my_plane == planes[0]
        if side is None:
            base_y = [(z_hi * HALF + lax.rem(y + k, HALF)) * NZ for k in range(HALF)]
        else:
            base_y = [(z_hi * HALF + side * 2 + lax.rem(y + k, 2)) * NZ for k in range(2)]
            at_home = at_home & (y // 2 == side)
        base_z = [lax.rem(me[2] + k, NZ) for k in range(NZ)]
        bases = [(x, y) for y in base_y for x in base_x]
        count = len(bases) * NZ
        for n in range(count):
            step = n * STRIDE % count
            x, y = bases[step % len(bases)]
            yield (at_home if step == 0 else None), x + y + base_z[step // len(bases)]

    def visit(planes, act, first=(), side=None):
        for there in first:
            pl.when(my_dev != there)(lambda: act(jnp.int32(there)))
        for self_at, there in members(planes, side):
            go = None if self_at is None else not_(self_at)
            for known in first:
                go = there != known if go is None else go & (there != known)
            if go is None:
                act(there)
            else:
                pl.when(go)(lambda: act(there))

    for load in loads:
        load.wait()
    weight[...] = volume[...] * jnp.exp(-LOG_STEP * exponent[...].astype(f32))
    y_layer[...] = weight[pl.ds(SPAN - 1, SPAN, stride=SPAN), :]
    last = one_hot(iota((8, LANES), 1) == LANES - 1)
    edge[...] = pick_t(last, weight[...])[0:1]

    @pl.when(is_root)
    def _():
        pl.semaphore_wait(barrier, DEV - 1)

    @pl.when(is_mid_root)
    def _():
        pl.semaphore_wait(barrier, DEV // 4 * 3 - 1)

    @pl.when(is_early_root)
    def _():
        pl.semaphore_wait(barrier, DEV // 2 - 1)

    @pl.when(not_(is_root | is_mid_root | is_early_root))
    def _():
        pl.semaphore_wait(barrier, len(HALO))

    halo_from = (
        weight.at[pl.ds(ROWS - SPAN, SPAN)], y_layer, weight.at[pl.ds(ROWS - 8, 8)],
        edge, edge, edge, edge,
    )
    halo_to = (
        lines_got.at[pl.ds(0, SPAN)], lines_got.at[pl.ds(SPAN, SPAN)],
        lines_got.at[pl.ds(2 * SPAN, 8)], *(z_got.at[n] for n in range(4)),
    )
    halos = []
    for n, step in enumerate(HALO):
        copy = pltpu.make_async_remote_copy(
            src_ref=halo_from[n], dst_ref=halo_to[n],
            send_sem=halo_send.at[n], recv_sem=halo_recv.at[n],
            device_id=ahead(*step), device_id_type=LOGICAL,
        )
        copy.start()
        halos.append(copy)

    @pl.when(is_early_root)
    def _():
        visit((0, 1), lambda there: signal(early_sem, there))

    @pl.when(is_mid_root)
    def _():
        visit((0, 1), lambda there: signal(mid_sem, there), FIRST)
        visit((2,), lambda there: signal(mid_sem, there))

    @pl.when(is_root)
    def _():
        visit((3,), lambda there: signal(go_sem, there))
        visit((0, 1), lambda there: signal(go_sem, there), FIRST)
        visit((2,), lambda there: signal(go_sem, there))

    owner_dev = owner[...] // ROWS
    slots = (owner[...] - owner_dev * ROWS).astype(f32)
    same = owner_dev == iota((DEV, ROWS), 0)
    before = one_hot(iota((ROWS, ROWS), 0) < iota((ROWS, ROWS), 1))
    rank = dot_n(one_hot(same), before)
    ranked = [one_hot(same & (rank == value)) for value in (0.0, 1.0)]
    order = jnp.concatenate(ranked, axis=0)

    def put(part, rows):
        packed[2 * part] = rows[:DEV]
        packed[2 * part + 1] = rows[DEV:]

    own = weight[...].reshape(SPAN, SPAN, LANES)
    put(0, pick(order, weight[...]))

    def send(first, count):
        def act(there):
            pltpu.make_async_remote_copy(
                src_ref=packed.at[pl.ds(first, count), pl.ds(there, 1), :],
                dst_ref=got.at[pl.ds(first, count), pl.ds(my_dev, 1), :],
                send_sem=send_sem, recv_sem=recv_sem,
                device_id=there, device_id_type=LOGICAL,
            ).start()

        return act

    empty = jnp.zeros((1, SPAN, LANES), f32)
    behind_x = jnp.concatenate([empty, own[:-1]], axis=0)
    column = jnp.zeros((SPAN, 1, LANES), f32)
    behind_y = jnp.concatenate([column, own[:, :-1]], axis=1)
    behind_xy = jnp.concatenate([column, behind_x[:, :-1]], axis=1)
    from_row, line = iota((ROWS, LANES), 0), iota((ROWS, LANES), 1)
    in_x, in_y = line < SPAN, (line >= SPAN) & (line < 2 * SPAN)
    wanted = (
        jnp.where(in_x, line, -1),
        jnp.where(in_y, (line - SPAN) * SPAN, -1),
        jnp.where(
            in_x & (line < SPAN - 1),
            line + 1,
            jnp.where(
                in_y & (line < 2 * SPAN - 1),
                (line - SPAN + 1) * SPAN,
                jnp.where(line == 2 * SPAN + 7, 0, -1),
            ),
        ),
    )
    selects = []
    for n, inner in enumerate((behind_x, behind_y, behind_xy)):
        put(n + 1, pick(order, inner.reshape(ROWS, LANES)))
        selects.append(dot_n(order, one_hot(from_row == wanted[n])).astype(bf16))
    select = jnp.concatenate(selects, axis=0)
    select = jnp.concatenate([select, select], axis=1)

    halos[0].wait()
    pad = jnp.zeros((LANES - SPAN, LANES), f32)
    x_lines = jnp.concatenate([lines_got[0:SPAN], pad], axis=0)
    rim = dot_n(select[:ROWS], jnp.concatenate(pieces(x_lines), axis=0))
    for n in range(2):
        packed[n + 2] += rim[n * DEV : (n + 1) * DEV]

    @pl.when(is_early & not_(is_early_root))
    def _():
        pl.semaphore_wait(early_sem, 1)

    @pl.when(is_mid & not_(is_mid_root))
    def _():
        pl.semaphore_wait(mid_sem, 1)

    @pl.when(is_late & not_(is_root))
    def _():
        pl.semaphore_wait(go_sem, 1)

    visit((0, 1), send(0, 4), FIRST)

    @pl.when(is_early & not_(is_mid_root))
    def _():
        pl.semaphore_wait(mid_sem, 1)

    visit((2,), send(0, 4))

    @pl.when(not_(is_late))
    def _():
        pl.semaphore_wait(go_sem, 1)

    visit((3,), send(0, 4))


    for copy in halos[1:]:
        copy.wait()

    pad = jnp.zeros((LANES - 2 * SPAN - 8, LANES), f32)
    rim_lines = jnp.concatenate([lines_got[...], pad], axis=0)
    rim = dot_n(select[ROWS:], jnp.concatenate(pieces(rim_lines), axis=0))
    for n in range(4):
        packed[n + 4] += rim[n * DEV : (n + 1) * DEV]

    at = iota((1, ROWS), 1)
    first_x, first_y = at < SPAN, at % SPAN == 0
    z_own, z_x, z_y, z_xy = (z_got[n] for n in range(4))

    def turn(row, by):
        return pltpu.roll(row, by % ROWS, 1)

    z_rows = (
        z_own,
        jnp.where(first_x, turn(z_x, SPAN), turn(z_own, SPAN)),
        jnp.where(first_y, turn(z_y, 1 - SPAN), turn(z_own, 1)),
        jnp.where(
            first_x,
            jnp.where(first_y, turn(z_xy, 1), turn(z_x, SPAN + 1)),
            jnp.where(first_y, turn(z_y, 1), turn(z_own, SPAN + 1)),
        ),
        slots,
    )
    table = jnp.zeros((8, ROWS), f32)
    for n, row in enumerate(z_rows):
        table = jnp.where(iota((8, ROWS), 0) == n, row, table)
    high, low = pieces(table)
    none = jnp.zeros((16, ROWS), bf16)
    blank = jnp.zeros((LANES - 32, ROWS), bf16)
    both = jnp.concatenate([high, low], axis=0)
    packed[8] = dot_t(ranked[0], jnp.concatenate([both, none, blank], axis=0)) + dot_t(
        ranked[1], jnp.concatenate([none, both, blank], axis=0)
    )

    keep = pltpu.make_async_copy(
        packed.at[:, pl.ds(my_dev, 1), :], got.at[:, pl.ds(my_dev, 1), :], own_sem
    )
    keep.start()
    visit((0, 1), send(4, PARTS - 4), FIRST)

    visit((2,), send(4, PARTS - 4))

    visit((3,), send(4, PARTS - 4))
    keep.wait()
    all_others = pl.ds(0, DEV - 1)
    pltpu.make_async_remote_copy(
        src_ref=packed.at[:, all_others], dst_ref=got.at[:, all_others],
        send_sem=send_sem, recv_sem=recv_sem, device_id=my_dev, device_id_type=LOGICAL,
    ).wait()


def assemble(got, stencil_hbm, lumped_hbm, stencil, lumped, out_sems, lump_sem):
    rows = ROWS // CHUNKS
    extra = got[8]
    extra += pltpu.roll(extra, LANES - 8, 1)
    tails = [extra, pltpu.roll(extra, LANES - 16, 1)]
    slot = jnp.concatenate(
        [
            dot_t(one_hot(iota((8, LANES), 1) == 4), tail.astype(bf16))[0:1]
            for tail in tails
        ],
        axis=1,
    )
    five = [(got[2 * n], got[2 * n + 1]) for n in range(4)] + [tails]
    five = [jnp.concatenate(pieces(jnp.concatenate(two, axis=0)), axis=1) for two in five]
    lane = iota((rows, LANES), 1)
    copies = []
    for chunk in range(CHUNKS):
        here = pl.ds(chunk * rows, rows)
        mine = iota((rows, ROWS), 0) + chunk * rows
        place = one_hot(slot == mine.astype(f32), 0.015625)
        both = [dot_n(place, two) for two in five]
        placed = [pair[:, :LANES] + pair[:, LANES:] for pair in both]
        now, tail = placed[:4], placed[4]
        behind = [
            jnp.where(lane == 0, tail[:, n : n + 1], pltpu.roll(line, 1, 1))
            for n, line in enumerate(now)
        ]
        total = sum(now) + sum(behind)
        lumped[here, :] = 1.0 / (27.0 * total)

        def spread(current, back):
            return (back, 2.0 * (current + back), current)

        def plane(four):
            along = zip(spread(four[0], four[1]), spread(four[2], four[3]))
            return [value for current, back in along for value in spread(current, back)]

        for n, (current, back) in enumerate(zip(plane(now), plane(behind))):
            for k, value in enumerate(spread(current, back)):
                stencil[3 * n + k, here, :] = value
        copy = pltpu.make_async_copy(
            stencil.at[:, here], stencil_hbm.at[:, here], out_sems.at[chunk]
        )
        copy.start()
        copies.append(copy)
    copy = pltpu.make_async_copy(lumped, lumped_hbm, lump_sem)
    copy.start()
    copies.append(copy)
    for copy in copies:
        copy.wait()


def in_hbm(x):
    return pltpu.with_memory_space_constraint(x, pltpu.HBM)


def shards(cell_volume, exponent, owner_row):
    vmem = pl.BlockSpec(memory_space=pltpu.VMEM)
    hbm = pl.BlockSpec(memory_space=pltpu.HBM)
    dma, regular = pltpu.SemaphoreType.DMA, pltpu.SemaphoreType.REGULAR
    got = pl.pallas_call(
        exchange,
        name="exchange",
        out_shape=pltpu.VMEM((PARTS, DEV, LANES), f32),
        in_specs=[hbm] * 3,
        out_specs=vmem,
        scratch_shapes=[
            pltpu.VMEM((ROWS, LANES), f32),
            pltpu.VMEM((ROWS, LANES), i32),
            pltpu.VMEM((1, ROWS), i32),
            pltpu.VMEM((ROWS, LANES), f32),
            pltpu.VMEM((SPAN, LANES), f32),
            pltpu.VMEM((1, ROWS), f32),
            pltpu.VMEM((2 * SPAN + 8, LANES), f32),
            pltpu.VMEM((4, 1, ROWS), f32),
            pltpu.VMEM((PARTS, DEV, LANES), f32),
            dma((3,)), dma((7,)), dma((7,)), dma, dma, dma, regular, regular, regular,
        ],
        compiler_params=pltpu.CompilerParams(
            has_side_effects=True, collective_id=1, vmem_limit_bytes=16 << 20
        ),
    )(
        in_hbm(cell_volume.reshape(ROWS, LANES)),
        in_hbm(exponent.reshape(ROWS, LANES)),
        in_hbm(owner_row.reshape(1, ROWS)),
    )
    return pl.pallas_call(
        assemble,
        name="assemble",
        out_shape=(
            jax.ShapeDtypeStruct((27, ROWS, LANES), f32),
            jax.ShapeDtypeStruct((ROWS, LANES), f32),
        ),
        in_specs=[vmem],
        out_specs=(hbm, hbm),
        scratch_shapes=[
            pltpu.VMEM((27, ROWS, LANES), f32),
            pltpu.VMEM((ROWS, LANES), f32),
            dma((CHUNKS,)), dma,
        ],
        compiler_params=pltpu.CompilerParams(vmem_limit_bytes=16 << 20),
    )(got)


def solution(mesh):
    return jax.shard_map(
        shards,
        mesh=mesh,
        in_specs=(P(*AXES), P(*AXES), P(AXES)),
        out_specs=(P(None, AXES, None), P(AXES, None)),
        check_vma=False,
    )
```
